32 devices in a mesh: group: 2 (over y), plane: 4 (over z), planey: 2 (over x), ens: 2 (over core).
Axes of the slice: x: 2, y: 2, z: 4, core: 2. Of those that a mesh axis runs over, the one named last changes fastest.
Arguments:
- u_prior: float32 [8, 2, 10, 64, 256], P(('group', 'ens'), None, None, 'plane', 'planey'), parts along dimension 0, may hold values from -6 to 6
- friction_rows: int32 [8], P(('group', 'ens')), parts along dimension 0, may hold values from 0 to 15
- friction_table: float32 [32, 64, 256], P('group', 'plane', 'planey'), parts along dimension 0, may hold values from 0.3 to 3
- bed_fixed: int32 [64, 256], P('plane', 'planey'), may hold values from -536870912 to 536870911
- ice_mask: int32 [64, 256], P('plane', 'planey'), may hold values 0 or 1
Outputs:
- mean_velocity: float32 [4, 10, 64, 256], P('group', None, 'plane', 'planey'), parts along dimension 0
The draws below stay inside these ranges and needn't reach their ends.
There are 2 independent parts, one for each index of `group`. The reference program is written for one: setup_inputs(seed, part) draws one part's arguments, and reference() takes and returns one part's arrays. A program takes and returns all parts, laid end to end along the dimension named above; an argument that names none is the same for every part. Nothing has to cross between parts.
Inputs may be any that keep to these rules, and one draw needn't show every extreme that they name: `friction_rows`: each sample names one row of the friction table.
All inputs are finite; a program needn't handle non-finite values. No bound on the sum of `ice_mask` on one device may be relied on, other than what follows from the above.
Results may differ from the reference program's by a relative error of at most 0.0003.
Values sent between devices are 32-bit elements; how exact they have to be, the bound alone decides.
A program may use at most 64 MiB of HBM per device.

```python
import math
import jax
import jax.numpy as jnp
from jax import lax

NZ = 10
ITERS = 2
LEVELS = 16
SAMPLES = 4
NX = 64
NY = 256


def with_ends(drawn, rng, least, largest):
    spot = [jax.random.randint(jax.random.fold_in(rng, axis), (), 0, length) for axis, length in enumerate(drawn.shape)]
    main_axis = drawn.shape.index(max(drawn.shape))
    next_to = spot[:main_axis] + [(spot[main_axis] + 1) % drawn.shape[main_axis]] + spot[main_axis + 1:]
    return drawn.at[tuple(spot)].set(least).at[tuple(next_to)].set(largest)


def shard_levels(stream_key, dims, shards, smallest, top_value):
    factor_of, own = 1.0, jax.random.fold_in(stream_key, 6)
    for axis_at, blocks in shards:
        draws = jnp.exp(jax.random.uniform(jax.random.fold_in(own, axis_at), (blocks,), jnp.float32, smallest / len(shards), top_value / len(shards)))
        factor_of = factor_of * jnp.repeat(draws, dims[axis_at] // blocks).reshape([-1 if axis == axis_at else 1 for axis in range(len(dims))])
    return factor_of


def scatter_about(stream_key, shape, width, bound, split=(), kind=jnp.bfloat16):
    values = jax.random.normal(stream_key, shape, jnp.float32) * width
    if len(split) > 0:
        values = shard_levels(stream_key, shape, split, -0.22, 0.18) * values
    return jnp.clip(values, min=-bound, max=bound).astype(kind)


def setup_inputs(seed: int = 0, part: int = 0) -> dict:
    keys = jax.random.split(jax.random.key(seed), 6)
    own_keys = jax.random.split(jax.random.fold_in(keys[5], part), 6)
    return {
        "u_prior": scatter_about(own_keys[0], (SAMPLES, 2, NZ, NX, NY), 1.0, 6.0, ((0, 2), (3, 4), (4, 2)), jnp.float32),
        "friction_rows": with_ends(jax.random.randint(own_keys[1], (SAMPLES,), 0, LEVELS), jax.random.fold_in(own_keys[1], 1), 0, LEVELS - 1).astype(jnp.int32),
        "friction_table": jnp.clip(jnp.exp(math.log(3.0) - 2.3025851 * jax.random.uniform(own_keys[2], (LEVELS, NX, NY), jnp.float32) ** shard_levels(own_keys[2], (LEVELS, NX, NY), ((1, 4), (2, 2)), -0.2, 0.2)), 0.3, 3.0),
        "bed_fixed": with_ends(jax.random.randint(keys[3], (NX, NY), -536870912, 536870912), jax.random.fold_in(keys[3], 1), -536870912, 536870911).astype(jnp.int32),
        "ice_mask": with_ends((jax.random.randint(keys[4], (NX, NY), 0, 8) < 7).astype(jnp.int32), jax.random.fold_in(keys[4], 1), 0, 1),
    }


bed_unit = 2.0 ** -29
factor_u = (2.0, 1.0, 0.5)
factor_v = (2.0, 0.5, 1.0)


def coefficient(offset):
    nonzero = len([entry for entry in offset if entry != 0])
    weight_u = 0.25 ** (nonzero - 1)
    weight_v = weight_u
    for dimension in range(3):
        if offset[dimension] != 0:
            weight_u = weight_u * factor_u[dimension]
            weight_v = weight_v * factor_v[dimension]
    return jnp.array([weight_u, weight_v], jnp.float32).reshape(2, 1, 1, 1)


def neighbour_sum(padded):
    layers = padded.shape[-3] - 2
    span_x = padded.shape[-2] - 2
    span_y = padded.shape[-1] - 2
    summed = None
    for step_z in (-1, 0, 1):
        for step_x in (-1, 0, 1):
            for step_y in (-1, 0, 1):
                if step_z == 0 and step_x == 0 and step_y == 0:
                    continue
                window = padded[..., 1 + step_z:1 + step_z + layers, 1 + step_x:1 + step_x + span_x, 1 + step_y:1 + step_y + span_y]
                addend = coefficient((step_z, step_x, step_y)) * window
                summed = addend if summed is None else summed + addend
    return summed


def strain_roots(extended):
    padded = jnp.pad(extended, [(0, 0)] * (extended.ndim - 3) + [(1, 1), (0, 0), (0, 0)])
    along_x = (padded[..., 1:-1, 2:, 1:-1] - padded[..., 1:-1, :-2, 1:-1]) * 0.5
    along_y = (padded[..., 1:-1, 1:-1, 2:] - padded[..., 1:-1, 1:-1, :-2]) * 0.5
    along_z = (padded[..., 2:, 1:-1, 1:-1] - padded[..., :-2, 1:-1, 1:-1]) * 0.5
    stretch_x = along_x[..., 0, :, :, :]
    stretch_y = along_y[..., 1, :, :, :]
    shear_one = along_y[..., 0, :, :, :]
    shear_two = along_x[..., 1, :, :, :]
    vertical_u = along_z[..., 0, :, :, :]
    vertical_v = along_z[..., 1, :, :, :]
    shear = shear_one + shear_two
    strain = stretch_x * stretch_x + stretch_y * stretch_y + stretch_x * stretch_y + 0.25 * shear * shear + 0.25 * (vertical_u * vertical_u + vertical_v * vertical_v)
    return jnp.power(strain + 0.1, -1.0 / 6.0)[..., None, :, :, :]


def reference(u_prior, friction_rows, friction_table, bed_fixed, ice_mask):
    cover = ice_mask.astype(jnp.float32)
    bed = bed_fixed.astype(jnp.float32) * bed_unit
    bed_pad = jnp.pad(bed, 1)
    slope_x = (bed_pad[2:, 1:-1] - bed_pad[:-2, 1:-1]) * 0.5
    slope_y = (bed_pad[1:-1, 2:] - bed_pad[1:-1, :-2]) * 0.5
    thickness = 1.0 + 2.0 * jnp.arange(NX, dtype=jnp.float32)[:, None] / (NX - 1)
    force = jnp.stack([-(cover * thickness * slope_x), -(cover * thickness * slope_y)])[:, None, :, :]
    bottom = (jnp.arange(NZ, dtype=jnp.int32) == 0).astype(jnp.float32)[:, None, None]
    levels = jnp.arange(LEVELS, dtype=jnp.int32)

    def solve(summed, inputs):
        prior, table_row = inputs
        extended = jnp.pad(prior, ((0, 0), (0, 0), (1, 1), (1, 1)))
        roots = cover * strain_roots(extended)
        across = neighbour_sum(jnp.pad(roots, ((0, 0), (1, 1), (1, 1), (1, 1))))
        chosen = (levels == table_row).astype(jnp.float32)
        friction = jnp.sum(chosen[:, None, None] * friction_table, axis=0)
        diag = cover * friction * bottom + (1.0 - cover)

        def operate(field):
            product = roots * field
            nearby = neighbour_sum(jnp.pad(product, ((0, 0), (1, 1), (1, 1), (1, 1))))
            return roots * (across * field - nearby) + diag * field

        solution = prior * cover
        residual = force - operate(solution)
        direction = residual
        norm_now = jnp.sum(residual * residual)
        for step in range(ITERS):
            image = operate(direction)
            alpha = norm_now / jnp.sum(direction * image)
            solution = solution + alpha * direction
            if step + 1 < ITERS:
                residual = residual - alpha * image
                norm_next = jnp.sum(residual * residual)
                direction = residual + (norm_next / norm_now) * direction
                norm_now = norm_next
        return summed + solution, None

    start = jnp.zeros((2, NZ, NX, NY), jnp.float32)
    summed = lax.scan(solve, start, (u_prior, friction_rows))[0]
    return summed / SAMPLES
```

```python
import functools
import jax
import jax.numpy as jnp
from jax import lax
from jax.experimental import pallas as pl
from jax.experimental.pallas import tpu as pltpu
from jax.sharding import PartitionSpec as P

bed_unit = 2.0 ** (-29)
HALO = 4
SLOTS = 16
STEP_I = (0.25, 0.125)
STEP_J = (0.125, 0.25)


def iota(shape, dim):
    return lax.broadcasted_iota(jnp.int32, shape, dim)


def shift_i(x, step):
    return pltpu.roll(x, (-step) % x.shape[-2], x.ndim - 2)


def shift_j(x, step):
    rolled = pltpu.roll(x, (-step) % x.shape[-1], x.ndim - 1)
    swapped = jnp.concatenate([rolled[1:2], rolled[0:1]], axis=0)
    lane = iota(x.shape, x.ndim - 1)
    edge = 0 if step < 0 else x.shape[-1] - 1
    return jnp.where(lane == edge, swapped, rolled)


def spread_ij(x, c):
    x = x + STEP_I[c] * (shift_i(x, 1) + shift_i(x, -1))
    return x + STEP_J[c] * (shift_j(x, 1) + shift_j(x, -1))


def spread_z(ref, index, z):
    return ref[index + (z + 1,)] + 0.5 * (ref[index + (z,)] + ref[index + (z + 2,)])


def chunk_places(members, layers):
    chunks, places, pair, group = [], [], 0, 0
    for m in range(members):
        base = 2 + members if m == 0 else 0
        base_even = base + base % 2
        count = base_even + 2 * layers
        pairs, groups = count // 2, (count + SLOTS - 1) // SLOTS
        chunks.append((pair, pairs, group, groups))
        places.append(base_even)
        pair, group = pair + pairs, group + groups
    return chunks, places


def kernel(sizes, rows_hbm, u_hbm, table_hbm, bed_hbm, mask_hbm, out_ref,
           rows_ref, u_v, table_v, bed_v, mask_v,
           up_s, down_s, side_s, corner_s,
           below_r, above_r, side_r, corner_r, hx,
           ext, roots, tr, pa, pb, r_ext, a_ext, force,
           r_core, a_core, w_core, r_peer, a_peer, w_peer,
           gram_s, gram_r,
           relay, in_sem, halo_send, halo_recv, peer_send, peer_recv, gram_send, gram_recv):
    np_, nq, ne = sizes
    members, _, layers, rows, cols = u_v.shape
    ring = rows + 2 * HALO
    ix, iy, ie = lax.axis_index("plane"), lax.axis_index("planey"), lax.axis_index("ens")

    total = np_ * nq * ne
    mesh_id = pl.DeviceIdType.MESH

    adjacent = []
    for dx in (0, -1, 1):
        for dy in (0, -1, 1):
            for de in range(ne):
                if (dx, dy, de) == (0, 0, 0):
                    continue
                tx, ty = ix + dx, iy + dy
                ok = (tx >= 0) & (tx < np_) & (ty >= 0) & (ty < nq)
                where = {"plane": jnp.clip(tx, 0, np_ - 1), "planey": jnp.clip(ty, 0, nq - 1),
                         "ens": lax.rem(ie + de, ne)}
                adjacent.append((ok, where))
    span_x = 1 + (ix > 0).astype(jnp.int32) + (ix < np_ - 1).astype(jnp.int32)
    span_y = 1 + (iy > 0).astype(jnp.int32) + (iy < nq - 1).astype(jnp.int32)
    adjacent_count = span_x * span_y * ne - 1
    rounds = max(max(np_, nq) - 2, 0)

    def signal_adjacent(sem):
        for ok, where in adjacent:
            @pl.when(ok)
            def _(where=where):
                pl.semaphore_signal(sem, inc=1, device_id=where, device_id_type=mesh_id)

    barrier = pltpu.get_barrier_semaphore()
    signal_adjacent(barrier)

    loads = [
        pltpu.make_async_copy(src, dst, in_sem.at[i])
        for i, (src, dst) in enumerate(
            ((u_hbm, u_v), (table_hbm, table_v), (bed_hbm, bed_v), (mask_hbm, mask_v),
             (rows_hbm, rows_ref))
        )
    ]
    for load in loads:
        load.start()

    def group_target(d):
        de, rest = d // (np_ * nq), d % (np_ * nq)
        return {
            "plane": lax.rem(ix + rest // nq, np_),
            "planey": lax.rem(iy + rest % nq, nq),
            "ens": lax.rem(ie + de, ne),
        }

    def each_peer(fn):
        if total <= 32:
            for d in range(1, total):
                fn(d)
        else:
            def step(d, carry):
                fn(d)
                return carry
            lax.fori_loop(1, total, step, 0)

    shared = [
        lambda: bed_v[...].astype(jnp.float32) * bed_unit,
        lambda: mask_v[...].astype(jnp.float32),
    ] + [(lambda m=m: table_v[rows_ref[m]]) for m in range(members)]
    if len(shared) % 2:
        shared.append(shared[-1])
    chunks, places = chunk_places(members, layers)
    readers = [
        (shared if m == 0 else [])
        + [(lambda m=m, c=c, z=z: u_v[m, c, z]) for z in range(layers) for c in range(2)]
        for m in range(members)
    ]

    flows = [[] for _ in chunks]
    absent = []
    for i, (dx, dy, src, dst) in enumerate((
        (-1, 0, up_s, below_r),
        (1, 0, down_s, above_r),
        (0, -1, side_s, side_r.at[1]),
        (0, 1, side_s, side_r.at[0]),
        (-1, -1, corner_s, corner_r.at[0, 1]),
        (-1, 1, corner_s, corner_r.at[0, 0]),
        (1, -1, corner_s, corner_r.at[1, 1]),
        (1, 1, corner_s, corner_r.at[1, 0]),
    )):
        tx, ty = ix + dx, iy + dy
        sx, sy = ix - dx, iy - dy
        to_ok = (tx >= 0) & (tx < np_) & (ty >= 0) & (ty < nq)
        from_ok = (sx >= 0) & (sx < np_) & (sy >= 0) & (sy < nq)
        absent.append((jnp.logical_not(from_ok), dst))
        for k, (pair, pairs, group, groups) in enumerate(chunks):
            part = pl.ds(pair, pairs) if i < 2 else pl.ds(group, groups)
            copy = pltpu.make_async_remote_copy(
                src_ref=src.at[part], dst_ref=dst.at[part],
                send_sem=halo_send.at[8 * k + i], recv_sem=halo_recv.at[8 * k + i],
                device_id={"plane": jnp.clip(tx, 0, np_ - 1), "planey": jnp.clip(ty, 0, nq - 1)},
                device_id_type=mesh_id)
            flows[k].append((copy, to_ok, from_ok))

    for load in loads:
        load.wait()

    low8 = iota((8, cols), 0) < 4
    lane_x = iota((rows, cols), 1)

    def ends(value):
        return jnp.where(low8, value[0:8], value[rows - 8:rows])

    for (pair, pairs, group, groups), read in zip(chunks, readers):
        for g in range(groups):
            packed = jnp.zeros((rows, cols), jnp.float32)
            for k in range(min(SLOTS, len(read) - g * SLOTS)):
                rolled = pltpu.roll(read[g * SLOTS + k](), (8 * k + 4) % cols, 1)
                packed = jnp.where((lane_x // 8) == k, rolled, packed)
            side_s[group + g] = packed
            corner_s[group + g] = ends(packed)
        for i in range(pairs):
            first = ends(read[2 * i]())
            turned = pltpu.roll(ends(read[min(2 * i + 1, len(read) - 1)]()), 4, 0)
            up_s[pair + i] = jnp.where(low8, first, turned)
            down_s[pair + i] = jnp.where(low8, turned, first)

    pl.semaphore_wait(barrier, adjacent_count)
    for chunk in flows:
        for copy, to_ok, from_ok in chunk:
            pl.when(to_ok)(copy.start)
    if rounds > 0:
        signal_adjacent(relay.at[0])

    for gone, dst in absent:
        @pl.when(gone)
        def _(dst=dst):
            dst[...] = jnp.zeros(dst.shape, jnp.float32)
    zero = jnp.zeros((2, ring, cols), jnp.float32)
    for m in range(members):
        for end in (0, layers + 1):
            roots[m, end] = zero
            for c in range(2):
                ext[m, c, end] = zero
                pa[m, c, end] = zero
                pb[m, c, end] = zero
    cover_core = mask_v[...].astype(jnp.float32)
    for c in range(2):
        for z in range(layers):
            summed = u_v[0, c, z]
            for m in range(1, members):
                summed = summed + u_v[m, c, z]
            w_core[c, z] = cover_core * summed

    def arrive(k):
        for copy, to_ok, from_ok in flows[k]:
            pl.when(from_ok)(copy.wait_recv)
        _, _, group, groups = chunks[k]
        for g in range(group, group + groups):
            hx[g, 0:rows] = jnp.where(lane_x % 8 < 4, side_r[0, g], side_r[1, g])
            left = jnp.where(low8, corner_r[0, 0, g], corner_r[1, 0, g])
            right = jnp.where(low8, corner_r[0, 1, g], corner_r[1, 1, g])
            hx[g, rows:ring] = jnp.where(lane_x[0:8] % 8 < 4, left, right)

    def extended(k, p):
        pair, _, group, _ = chunks[k]
        i = pair + p // 2
        if p % 2 == 0:
            tail = jnp.where(low8, below_r[i], above_r[i])
        else:
            tail = pltpu.roll(jnp.where(low8, above_r[i], below_r[i]), 4, 0)
        core = jnp.concatenate([readers[k][p](), tail], axis=0)
        halo = pltpu.roll(hx[group + p // SLOTS], (-(8 * (p % SLOTS) + 4)) % cols, 1)
        return jnp.stack([core, halo])

    def assemble(m):
        arrive(m)
        base = places[m]
        for z in range(layers):
            for c in range(2):
                ext[m, c, z + 1] = extended(m, base + 2 * z + c)
        if m > 0:
            return
        bed = extended(0, 0)
        cover = extended(0, 1)
        row = iota((2, ring, cols), 1)
        position = (ix * rows + jnp.where(row < rows + HALO, row, row - ring)).astype(jnp.float32)
        thickness = 1.0 + 2.0 * position / (np_ * rows - 1)
        slope_x = (shift_i(bed, 1) - shift_i(bed, -1)) * 0.5
        slope_y = (shift_j(bed, 1) - shift_j(bed, -1)) * 0.5
        force[0] = -(cover * thickness * slope_x)
        force[1] = -(cover * thickness * slope_y)
        force[2] = cover
        force[3 + members] = 2.0 * cover
        for k in range(members):
            force[3 + k] = cover * extended(0, 2 + k)

    def roots_step(m, z):
        u, v = ext[m, 0, z + 1], ext[m, 1, z + 1]
        u_i = (shift_i(u, 1) - shift_i(u, -1)) * 0.5
        v_j = (shift_j(v, 1) - shift_j(v, -1)) * 0.5
        shear = ((shift_j(u, 1) - shift_j(u, -1)) + (shift_i(v, 1) - shift_i(v, -1))) * 0.5
        u_z = (ext[m, 0, z + 2] - ext[m, 0, z]) * 0.5
        v_z = (ext[m, 1, z + 2] - ext[m, 1, z]) * 0.5
        strain = (u_i * u_i + v_j * v_j + u_i * v_j + 0.25 * shear * shear
                  + 0.25 * (u_z * u_z + v_z * v_z))
        root = force[3 + members] * jnp.exp(jnp.log(strain + 0.1) * (-1.0 / 6.0))
        roots[m, z + 1] = root
        pa[m, 0, z + 1] = root * u
        pa[m, 1, z + 1] = root * v

    def image(m, c, z, field, p_ref):
        spread = spread_ij(spread_z(p_ref, (m, c), z), c)
        return tr[m, c, z] * field - roots[m, z + 1] * spread

    def residual_step(m, z, acc):
        near = spread_z(roots, (m,), z)
        diag = 1.0 - force[2]
        if z == 0:
            diag = diag + force[3 + m]
        for c in range(2):
            tr[m, c, z] = roots[m, z + 1] * spread_ij(near, c) + diag
            r = force[c] - image(m, c, z, force[2] * ext[m, c, z + 1], pa)
            r_ext[m, c, z] = r
            pb[m, c, z + 1] = roots[m, z + 1] * r
            core = r[0, 0:rows]
            r_core[m, c, z] = core
            acc = acc + core * core
        return acc

    def image_step(m, z, ra, aa):
        for c in range(2):
            r = r_ext[m, c, z]
            a = image(m, c, z, r, pb)
            a_ext[m, c, z] = a
            pa[m, c, z + 1] = roots[m, z + 1] * a
            core = a[0, 0:rows]
            a_core[m, c, z] = core
            ra = ra + r[0, 0:rows] * core
            aa = aa + core * core
        return ra, aa

    def second_step(m, z, ab):
        for c in range(2):
            a = a_ext[m, c, z]
            b = image(m, c, z, a, pa)
            ab = ab + a[0, 0:rows] * b[0, 0:rows]
        return ab

    peer = {"ens": lax.rem(ie + 1, ne)}

    def to_peer(i, src, dst):
        return pltpu.make_async_remote_copy(
            src_ref=src, dst_ref=dst, send_sem=peer_send.at[i], recv_sem=peer_recv.at[i],
            device_id=peer, device_id_type=mesh_id)

    peer_flows = [to_peer(0, w_core, w_peer)]
    for m in range(members):
        peer_flows.append(to_peer(2 * m + 1, r_core.at[m], r_peer.at[m]))
        peer_flows.append(to_peer(2 * m + 2, a_core.at[m], a_peer.at[m]))

    zero_core = jnp.zeros((rows, cols), jnp.float32)
    grams = []
    for m in range(members):
        assemble(m)
        for z in range(layers):
            roots_step(m, z)
        if m == 0:
            peer_flows[0].start()
            for k in range(1, rounds):
                pl.semaphore_wait(relay.at[k - 1], adjacent_count)
                signal_adjacent(relay.at[k])
        rr = ra = aa = ab = zero_core
        for z in range(layers):
            rr = residual_step(m, z, rr)
        for z in range(layers):
            ra, aa = image_step(m, z, ra, aa)
        peer_flows[2 * m + 1].start()
        for z in range(layers):
            ab = second_step(m, z, ab)
        peer_flows[2 * m + 2].start()
        grams.append((rr, ra, aa, ab))

    lane_1 = iota((1, cols), 1)
    mine = jnp.zeros((1, cols), jnp.float32)
    for m in range(members):
        for q, acc in enumerate(grams[m]):
            value = jnp.sum(jnp.sum(acc, axis=0, keepdims=True), axis=1, keepdims=True)
            mine = jnp.where(lane_1 == 4 * m + q, value, mine)
    gram_s[0] = mine

    if rounds > 0:
        pl.semaphore_wait(relay.at[rounds - 1], adjacent_count)

    def gram_copy(d):
        return pltpu.make_async_remote_copy(
            src_ref=gram_s, dst_ref=gram_r.at[pl.ds(d, 1)],
            send_sem=gram_send, recv_sem=gram_recv,
            device_id=group_target(d), device_id_type=pl.DeviceIdType.MESH)

    each_peer(lambda d: gram_copy(d).start())
    everything = pltpu.make_async_remote_copy(
        src_ref=gram_r.at[pl.ds(1, total - 1)], dst_ref=gram_r.at[pl.ds(1, total - 1)],
        send_sem=gram_send, recv_sem=gram_recv,
        device_id=group_target(1), device_id_type=pl.DeviceIdType.MESH)
    everything.wait_recv()

    half = np_ * nq
    own = mine
    if half > 1:
        own = own + jnp.sum(gram_r[1:half], axis=0)
    sums = [own] + [jnp.sum(gram_r[half * e:half * (e + 1)], axis=0) for e in range(1, ne)]
    steps = []
    for e in range(ne):
        for m in range(members):
            g_rr, g_ra, g_aa, g_ab = [
                jnp.sum(jnp.where(lane_1 == 4 * m + q, sums[e], 0.0), axis=1, keepdims=True)
                for q in range(4)
            ]
            first = g_rr / g_ra
            following = g_rr - 2.0 * first * g_ra + first * first * g_aa
            growth = 1.0 + following / g_rr
            curve = (growth * growth * g_ra - 2.0 * growth * first * g_aa
                     + first * first * g_ab)
            second = following / curve
            share = 1.0 / (members * ne)
            steps.append(((first + second * growth) * share, second * first * share))

    for flow in peer_flows:
        flow.wait_recv()
    share = 1.0 / (members * ne)

    def final_step(z, carry):
        for c in range(2):
            value = share * (w_core[c, z] + w_peer[c, z])
            for m in range(members):
                value = value + steps[m][0] * r_core[m, c, z] - steps[m][1] * a_core[m, c, z]
                one, two = steps[members + m]
                value = value + one * r_peer[m, c, z] - two * a_peer[m, c, z]
            out_ref[c, z] = value
        return carry

    lax.fori_loop(0, layers, final_step, 0)

    for chunk in flows:
        for copy, to_ok, from_ok in chunk:
            pl.when(to_ok)(copy.wait_send)
    for flow in peer_flows:
        flow.wait_send()
    everything.wait_send()


def body(sizes, u_prior, friction_rows, friction_table, bed_fixed, ice_mask):
    members, _, layers, rows, cols = u_prior.shape
    levels = friction_table.shape[0]
    total = sizes[0] * sizes[1] * sizes[2]
    ring = rows + 2 * HALO
    chunks, _ = chunk_places(members, layers)
    pairs = sum(chunk[1] for chunk in chunks)
    groups = sum(chunk[3] for chunk in chunks)
    f32 = jnp.float32
    any_space = pl.BlockSpec(memory_space=pl.ANY)
    vmem = lambda *shape: pltpu.VMEM(shape, f32)
    core = (members, 2, layers, rows, cols)
    wide = (2, ring, cols)
    return pl.pallas_call(
        functools.partial(kernel, sizes),
        out_shape=pltpu.VMEM((2, layers, rows, cols), f32),
        in_specs=[any_space] * 5,
        out_specs=pl.BlockSpec(memory_space=pltpu.VMEM),
        scratch_shapes=[
            pltpu.SMEM((members,), jnp.int32), vmem(*core), vmem(levels, rows, cols),
            pltpu.VMEM((rows, cols), jnp.int32), pltpu.VMEM((rows, cols), jnp.int32),
            vmem(pairs, 8, cols), vmem(pairs, 8, cols), vmem(groups, rows, cols), vmem(groups, 8, cols),
            vmem(pairs, 8, cols), vmem(pairs, 8, cols), vmem(2, groups, rows, cols),
            vmem(2, 2, groups, 8, cols), vmem(groups, ring, cols),
            vmem(members, 2, layers + 2, *wide), vmem(members, layers + 2, *wide),
            vmem(members, 2, layers, *wide),
            vmem(members, 2, layers + 2, *wide), vmem(members, 2, layers + 2, *wide),
            vmem(members, 2, layers, *wide), vmem(members, 2, layers, *wide),
            vmem(4 + members, *wide),
            vmem(*core), vmem(*core), vmem(*core[1:]),
            vmem(*core), vmem(*core), vmem(*core[1:]),
            vmem(1, 1, cols), vmem(total, 1, cols),
            pltpu.SemaphoreType.REGULAR((max(sizes[0], sizes[1]),)),
            pltpu.SemaphoreType.DMA((5,)),
            pltpu.SemaphoreType.DMA((8 * members,)), pltpu.SemaphoreType.DMA((8 * members,)),
            pltpu.SemaphoreType.DMA((2 * members + 1,)), pltpu.SemaphoreType.DMA((2 * members + 1,)),
            pltpu.SemaphoreType.DMA, pltpu.SemaphoreType.DMA,
        ],
        compiler_params=pltpu.CompilerParams(
            collective_id=0, has_side_effects=True, vmem_limit_bytes=24 << 20),
        name="picard",
    )(*[pltpu.with_memory_space_constraint(x, pltpu.HBM) for x in (
        friction_rows, u_prior, friction_table, bed_fixed, ice_mask)])


def solution(mesh):
    sizes = (mesh.shape["plane"], mesh.shape["planey"], mesh.shape["ens"])
    in_specs = (
        P(("group", "ens"), None, None, "plane", "planey"),
        P(("group", "ens")),
        P("group", "plane", "planey"),
        P("plane", "planey"),
        P("plane", "planey"),
    )
    out_specs = P("group", None, "plane", "planey")
    return jax.shard_map(functools.partial(body, sizes), mesh=mesh, in_specs=in_specs,
                         out_specs=out_specs, check_vma=False)
```

```python
import functools
import math
import numpy as np
import jax
import jax.numpy as jnp
from jax import lax
from jax.experimental import pallas as pl
from jax.experimental.pallas import tpu as pltpu
from jax.sharding import PartitionSpec as P

bed_unit = 2.0 ** (-29)
HALO = 4
TOP = 8
SPAN = 24
TALL = 144
PAD = 160
STEP_I = (0.25, 0.125)
STEP_J = (0.125, 0.25)


def iota(shape, dim):
    return lax.broadcasted_iota(jnp.int32, shape, dim)


def turn(x, step):
    return pltpu.roll(x, step % x.shape[1], 1)


def stencils(layers, members, lanes):
    def matrix(entry):
        out = np.zeros((lanes, lanes), np.float32)
        for z in range(layers):
            for i in range(-HALO, SPAN - HALO):
                for dz in (-1, 0, 1):
                    for di in (-1, 0, 1):
                        if 0 <= z + dz < layers and -HALO <= i + di < SPAN - HALO:
                            out[(z + dz) * SPAN + (i + di) % SPAN, z * SPAN + i % SPAN] = entry(dz, di)
        return out

    def copies(slot, targets, steps):
        out = np.zeros((lanes, lanes), np.float32)
        for z in targets:
            for i in range(-HALO, SPAN - HALO):
                for di, weight in steps:
                    if -HALO <= i + di < SPAN - HALO:
                        out[slot * SPAN + (i + di) % SPAN, z * SPAN + i % SPAN] = weight
        return out

    same, difference = ((0, 1.0),), ((1, 1.0), (-1, -1.0))
    every = range(layers)
    out = [matrix(lambda dz, di, c=c: (2.0 - abs(dz)) * (STEP_I[c] if di else 1.0)) for c in range(2)]
    out.append(matrix(lambda dz, di: 0.0 if dz else float(di)))
    out.append(matrix(lambda dz, di: 0.0 if di else float(dz)))
    out += [copies(1, every, same), copies(0, every, same), copies(0, every, difference)]
    out += [copies(2 + m, (0,), same) for m in range(members)]
    return np.stack(out)


def kernel(sizes, rows_hbm, u_hbm, table_hbm, bed_hbm, mask_hbm, matrix_hbm, out_ref,
           rows_ref, flat, table_v, bed_v, mask_v, matrix,
           up_s, down_s, side_s, corner_s,
           below_r, above_r, side_r, corner_r,
           tall, cover, roots, tr, pa, pb, r_ext, a_ext, force,
           w_core, r_core, a_core, r_peer, a_peer, w_peer, gram_s, gram_r, blank, wide_blank,
           relay, in_sem, halo_send, halo_recv, peer_send, peer_recv, gram_send, gram_recv):
    np_, nq, ne = sizes
    members, _, layers, rows, cols = u_hbm.shape
    ix, iy, ie = lax.axis_index("plane"), lax.axis_index("planey"), lax.axis_index("ens")
    total = np_ * nq * ne
    mesh_id = pl.DeviceIdType.MESH
    fixed = 2 + members
    lanes = 2 * cols
    assert rows + 2 * HALO == SPAN and cols == 128 and layers * SPAN <= lanes and fixed <= layers
    other = 2 * members

    loads = [
        pltpu.make_async_copy(src, dst, in_sem.at[i])
        for i, (src, dst) in enumerate(
            [(u_hbm.at[m], flat.at[pl.ds(2 * m, 2), pl.ds(0, layers), pl.ds(0, rows)])
             for m in range(members)]
            + [(table_hbm, table_v), (bed_hbm, bed_v), (mask_hbm, mask_v), (rows_hbm, rows_ref),
               (matrix_hbm, matrix)])
    ]
    for load in loads:
        load.start()
    late = loads.pop()

    adjacent = []
    for dx in (0, -1, 1):
        for dy in (0, -1, 1):
            for de in range(ne):
                if (dx, dy, de) == (0, 0, 0):
                    continue
                tx, ty = ix + dx, iy + dy
                ok = (tx >= 0) & (tx < np_) & (ty >= 0) & (ty < nq)
                where = {"plane": jnp.clip(tx, 0, np_ - 1), "planey": jnp.clip(ty, 0, nq - 1),
                         "ens": lax.rem(ie + de, ne)}
                adjacent.append((ok, where))
    span_x = 1 + (ix > 0).astype(jnp.int32) + (ix < np_ - 1).astype(jnp.int32)
    span_y = 1 + (iy > 0).astype(jnp.int32) + (iy < nq - 1).astype(jnp.int32)
    adjacent_count = span_x * span_y * ne - 1
    rounds = max(max(np_, nq) - 2, 0)

    def signal_adjacent(sem):
        for ok, where in adjacent:
            @pl.when(ok)
            def _(where=where):
                pl.semaphore_signal(sem, inc=1, device_id=where, device_id_type=mesh_id)

    barrier = pltpu.get_barrier_semaphore()
    signal_adjacent(barrier)

    def group_target(d):
        de, rest = d // (np_ * nq), d % (np_ * nq)
        return {
            "plane": lax.rem(ix + rest // nq, np_),
            "planey": lax.rem(iy + rest % nq, nq),
            "ens": lax.rem(ie + de, ne),
        }

    def each_peer(fn):
        if total <= 32:
            for d in range(1, total):
                fn(d)
        else:
            def step(d, carry):
                fn(d)
                return carry
            lax.fori_loop(1, total, step, 0)

    planes = [
        ([(other, k) for k in range(fixed + fixed % 2)] if m == 0 else [])
        + [(2 * m + c, z) for z in range(layers) for c in range(2)]
        for m in range(members)
    ]
    pair_at = [sum(len(p) for p in planes[:m]) // 2 for m in range(members)]
    pair_count = [len(p) // 2 for p in planes]
    side_tiles = [((2 * m, 2 * m + 1), m) for m in range(members)] + [((other,), 0)]
    tile_at = [[t for t, (_, k) in enumerate(side_tiles) if k == m] for m in range(members)]

    has_up, has_down = ix > 0, ix < np_ - 1
    has_left, has_right = iy > 0, iy < nq - 1
    rims, flanks = [[] for _ in planes], [[] for _ in planes]
    absent = []
    for dx, dy, src, dst in (
        (-1, -1, corner_s.at[0, 0], corner_r.at[1, 1]),
        (-1, 1, corner_s.at[0, 1], corner_r.at[1, 0]),
        (1, -1, corner_s.at[1, 0], corner_r.at[0, 1]),
        (1, 1, corner_s.at[1, 1], corner_r.at[0, 0]),
        (0, -1, side_s.at[0], side_r.at[1]),
        (0, 1, side_s.at[1], side_r.at[0]),
        (-1, 0, up_s, below_r),
        (1, 0, down_s, above_r),
    ):
        tx, ty = ix + dx, iy + dy
        sx, sy = ix - dx, iy - dy
        to_ok = (tx >= 0) & (tx < np_) & (ty >= 0) & (ty < nq)
        from_ok = (sx >= 0) & (sx < np_) & (sy >= 0) & (sy < nq)
        absent.append((jnp.logical_not(from_ok), dst))
        for k in range(members):
            if dy:
                parts = [pl.ds(t, 1) for t in tile_at[k]]
            elif k == 0:
                head = pair_count[0] // 2
                parts = [pl.ds(0, head), pl.ds(head, pair_count[0] - head)]
            else:
                parts = [pl.ds(pair_at[k], pair_count[k])]
            for part in parts:
                copy = pltpu.make_async_remote_copy(
                    src_ref=src.at[part], dst_ref=dst.at[part],
                    send_sem=halo_send, recv_sem=halo_recv.at[k],
                    device_id={"plane": jnp.clip(tx, 0, np_ - 1), "planey": jnp.clip(ty, 0, nq - 1)},
                    device_id_type=mesh_id)
                (flanks if dy else rims)[k].append((to_ok, copy))

    def tiles(count):
        return blank.at[pl.ds(0, count)]

    def settle(chunk_list, received):
        for up in (0, 1):
            for down in (0, 1):
                for left in (0, 1):
                    for right in (0, 1):
                        if (up + down > np_ - 1 or left + right > nq - 1
                                or (np_ > 1 and up + down == 0) or (nq > 1 and left + right == 0)):
                            continue
                        count = sum(
                            pair_count[k] * (up + down)
                            + len(tile_at[k]) * (2 + up + down) * (left + right) for k in chunk_list)
                        if count == 0:
                            continue
                        here = ((has_up == bool(up)) & (has_down == bool(down))
                                & (has_left == bool(left)) & (has_right == bool(right)))
                        bulk = pltpu.make_async_remote_copy(
                            src_ref=tiles(count), dst_ref=tiles(count), send_sem=halo_send,
                            recv_sem=halo_recv.at[chunk_list[0]],
                            device_id={"ens": lax.rem(ie + 1, ne)}, device_id_type=mesh_id)
                        pl.when(here)(bulk.wait_recv if received else bulk.wait_send)

    rim = jnp.zeros((SPAN - rows, cols), jnp.float32)
    for f in range(other + 1):
        flat[f, layers] = jnp.zeros((SPAN, cols), jnp.float32)
        for z in range(layers):
            flat[f, z, pl.ds(rows, SPAN - rows)] = rim
    for k in range(fixed, layers):
        flat[other, k, pl.ds(0, rows)] = jnp.zeros((rows, cols), jnp.float32)

    for load in loads:
        load.wait()

    cover_core = mask_v[...].astype(jnp.float32)
    flat[other, 0, pl.ds(0, rows)] = bed_v[...].astype(jnp.float32) * bed_unit
    flat[other, 1, pl.ds(0, rows)] = cover_core
    for m in range(members):
        flat[other, 2 + m, pl.ds(0, rows)] = table_v[rows_ref[m]]
    for m in range(members):
        for i, at in enumerate(planes[m]):
            half = pl.ds(HALO * (i % 2), HALO)
            up_s[pair_at[m] + i // 2, half] = flat[at + (pl.ds(0, HALO),)]
            down_s[pair_at[m] + i // 2, half] = flat[at + (pl.ds(rows - HALO, HALO),)]

    pl.semaphore_wait(barrier, adjacent_count)

    def send(chosen):
        for to_ok, copy in chosen:
            pl.when(to_ok)(copy.start)

    send(rims[0][0::2])

    lane8 = iota((8, cols), 1)

    def places(start, offset):
        out = None
        for z in range(layers):
            low = z * SPAN + start - offset
            if -HALO < low < cols:
                here = (lane8 >= low) & (lane8 < low + HALO)
                out = here if out is None else out | here
        return out

    def stood_up(f):
        plain = flat[f].reshape((layers + 1) * SPAN, cols)
        return [plain[cols * h:cols * (h + 1)].T for h in range(2)]

    for fields, k in side_tiles:
        edges = []
        for f in fields:
            halves = stood_up(f)
            edges.append([[half[start:start + HALO] for half in halves] for start in (0, cols - HALO)])
        if len(edges) == 1:
            edges.append([[jnp.zeros((HALO, cols), jnp.float32)] * 2] * 2)
        t = side_tiles.index((fields, k))
        for h in range(2):
            pair = [jnp.concatenate([edges[0][h][q], edges[1][h][q]], axis=0) for q in range(2)]
            side_s[h, t, 0] = pair[0]
            side_s[h, t, 1] = pair[1]
            corner_s[0, h, t] = jnp.where(places(0, 0), pair[0], pair[1])
            corner_s[1, h, t] = jnp.where(places(rows - HALO, 0), pair[0], pair[1])
    send(flanks[0])
    send(rims[0][1::2])
    for k in range(1, members):
        send(flanks[k])
        send(rims[k])
    if rounds > 0:
        signal_adjacent(relay.at[0])

    for gone, dst in absent:
        @pl.when(gone)
        def _(dst=dst):
            dst[...] = jnp.zeros(dst.shape, jnp.float32)
    for c in range(2):
        for z in range(layers):
            summed = flat[c, z, pl.ds(0, rows)]
            for m in range(1, members):
                summed = summed + flat[2 * m + c, z, pl.ds(0, rows)]
            w_core[c, z] = cover_core * summed

    peer = {"ens": lax.rem(ie + 1, ne)}

    def to_peer(src, dst):
        return pltpu.make_async_remote_copy(
            src_ref=src, dst_ref=dst, send_sem=peer_send, recv_sem=peer_recv,
            device_id=peer, device_id_type=mesh_id)

    send_w = to_peer(w_core, w_peer)
    send_r = [to_peer(r_core.at[m], r_peer.at[m]) for m in range(members)]
    send_a = [to_peer(a_core.at[m], a_peer.at[m]) for m in range(members)]
    send_w.start()

    def relay_on(k):
        pl.semaphore_wait(relay.at[k - 1], adjacent_count)
        signal_adjacent(relay.at[k])

    if rounds > 1:
        relay_on(1)
    late.wait()

    def at(ref, index, base, count=TALL):
        return ref[index + (pl.ds(base, count),)]

    def assemble(k):
        settle([k], True)
        for i, place in enumerate(planes[k]):
            half = pl.ds(HALO * (i % 2), HALO)
            pair = pair_at[k] + i // 2
            flat[place + (pl.ds(rows, HALO),)] = below_r[pair, half]
            flat[place + (pl.ds(rows + HALO, HALO),)] = above_r[pair, half]
        for t in tile_at[k]:
            for h in range(2):
                over = turn(corner_r[0, h, t], SPAN - rows)
                under = turn(corner_r[1, h, t], rows)
                whole = []
                for q in range(2):
                    part = jnp.where(places(rows + HALO, cols * q), over, side_r[h, t, q])
                    whole.append(jnp.where(places(rows, cols * q), under, part))
                start = TOP + cols if h else TOP - HALO
                for n, f in enumerate(side_tiles[t][0]):
                    for q in range(2):
                        tall[f, pl.ds(start, HALO), pl.ds(cols * q, cols)] = (
                            whole[q][HALO * n:HALO * (n + 1)])
            for f in side_tiles[t][0]:
                for q, half in enumerate(stood_up(f)):
                    tall[f, pl.ds(TOP, cols), pl.ds(cols * q, cols)] = half

    def split(x):
        high = x.astype(jnp.bfloat16)
        return [high, (x - high.astype(jnp.float32)).astype(jnp.bfloat16)]

    def times(k, *values):
        n = values[0].shape[0]
        out = jnp.dot(jnp.concatenate(sum([split(x) for x in values], []), axis=0), matrix[k],
                      preferred_element_type=jnp.float32)
        return [out[2 * n * i:2 * n * i + n] + out[2 * n * i + n:2 * n * i + 2 * n]
                for i in range(len(values))]

    root_base, res_base, img_base = TOP - 3, TOP - 2, TOP - 1
    lane = iota((8, lanes), 1)
    layer = sum([(lane >= SPAN * z).astype(jnp.int32) for z in range(1, layers + 1)])
    place = lane - SPAN * layer
    inside = ((place < rows) & (layer < layers)).astype(jnp.float32)[0:1]

    def prepare():
        b = res_base
        cover[pl.ds(root_base, TALL)] = jnp.dot(
            at(tall, (other,), root_base).astype(jnp.bfloat16), matrix[4],
            preferred_element_type=jnp.float32)

    def prepare_force():
        b = res_base
        row = (ix * rows + jnp.where(place < rows + HALO, place, place - SPAN))[0:1]
        thickness = 1.0 + 2.0 * row.astype(jnp.float32) / (np_ * rows - 1)
        covered = at(cover, (), b)
        field = at(tall, (other,), b)
        (slope_x,) = times(6, field)
        (slope_y,) = times(5, at(tall, (other,), b + 1) - at(tall, (other,), b - 1))
        force[0] = -(covered * thickness * (slope_x * 0.5))
        force[1] = -(covered * thickness * (slope_y * 0.5))
        for m in range(members):
            (friction,) = times(7 + m, field)
            force[2 + m] = (1.0 - covered) + covered * friction

    def roots_level(m):
        b = root_base
        u, v = at(tall, (2 * m,), b), at(tall, (2 * m + 1,), b)
        u_i, v_i = times(2, u, v)
        u_z, v_z = times(3, u, v)
        u_j = at(tall, (2 * m,), b + 1) - at(tall, (2 * m,), b - 1)
        v_j = at(tall, (2 * m + 1,), b + 1) - at(tall, (2 * m + 1,), b - 1)
        shear = u_j + v_i
        strain = (4.0 * (u_i * (u_i + v_j) + v_j * v_j) + shear * shear
                  + (u_z * u_z + v_z * v_z)) * 0.0625
        root = at(cover, (), b) * (
            math.sqrt(2.0) * jnp.exp(jnp.log(strain + 0.1) * (-1.0 / 6.0)))
        roots[m, pl.ds(b, TALL)] = root
        pa[m, 0, pl.ds(b, TALL)] = root * u
        pa[m, 1, pl.ds(b, TALL)] = root * v

    def lean(ref, index, base, c):
        return at(ref, index, base) + STEP_J[c] * (at(ref, index, base - 1) + at(ref, index, base + 1))

    def residual_level(m):
        b = res_base
        for c in range(2):
            near, moved = times(c, lean(roots, (m,), b, c), lean(pa, (m, c), b, c))
            root = at(roots, (m,), b)
            weight = root * near + force[2 + m]
            r = force[c] - (weight * (at(cover, (), b) * at(tall, (2 * m + c,), b)) - root * moved)
            tr[m, c, pl.ds(b, TALL)] = weight
            r_ext[m, c, pl.ds(b, TALL)] = r
            pb[m, c, pl.ds(b, TALL)] = root * r

    def image_level(m):
        b = img_base
        for c in range(2):
            (moved,) = times(c, lean(pb, (m, c), b, c))
            root = at(roots, (m,), b)
            a = at(tr, (m, c), b) * at(r_ext, (m, c), b) - root * moved
            a_ext[m, c, pl.ds(b, TALL)] = a
            pa[m, c, pl.ds(b, TALL)] = root * a

    def second_level(m):
        def fold(x):
            out = x[0:8]
            for start in range(8, cols, 8):
                out = out + x[start:start + 8]
            return out

        sums = [None] * 4
        for c in range(2):
            scaled = at(pa, (m, c), TOP, cols)
            (out,) = times(c, scaled + (2.0 * STEP_J[c]) * at(pa, (m, c), TOP - 1, cols))
            r, a = at(r_ext, (m, c), TOP, cols), at(a_ext, (m, c), TOP, cols)
            square = a * a
            terms = [fold(x) for x in (r * r, r * a, square,
                                       at(tr, (m, c), TOP, cols) * square - scaled * out)]
            sums = terms if c == 0 else [s + t for s, t in zip(sums, terms)]
        return [inside * jnp.sum(s, axis=0, keepdims=True) for s in sums]

    grams = []
    for m in range(members):
        assemble(m)
        if m == 0:
            prepare()
        roots_level(m)
        if m == 0:
            prepare_force()
        if m > 0:
            image_level(m - 1)
        residual_level(m)
        if m > 0:
            grams.append(second_level(m - 1))
        if m == 0:
            for k in range(2, rounds):
                relay_on(k)
    image_level(members - 1)
    grams.append(second_level(members - 1))

    lane_1 = iota((1, cols), 1)
    mine = jnp.zeros((1, cols), jnp.float32)
    for m in range(members):
        for q, acc in enumerate(grams[m]):
            mine = jnp.where(lane_1 == 4 * m + q, jnp.sum(acc, axis=1, keepdims=True), mine)
    gram_s[0] = mine

    if rounds > 0:
        pl.semaphore_wait(relay.at[rounds - 1], adjacent_count)

    def gram_copy(d):
        return pltpu.make_async_remote_copy(
            src_ref=gram_s, dst_ref=gram_r.at[pl.ds(d, 1)],
            send_sem=gram_send, recv_sem=gram_recv,
            device_id=group_target(d), device_id_type=pl.DeviceIdType.MESH)

    each_peer(lambda d: gram_copy(d).start())

    def lie_down(src, dst):
        for c in range(2):
            whole = src[c, pl.ds(TOP, cols)]
            flat_rows = jnp.concatenate(
                [whole[:, cols * q:cols * (q + 1)].T for q in range(2)], axis=0)
            for z in range(layers):
                dst[c, z] = flat_rows[SPAN * z:SPAN * z + rows]

    for m in range(members):
        lie_down(r_ext.at[m], r_core.at[m])
        send_r[m].start()
        lie_down(a_ext.at[m], a_core.at[m])
        send_a[m].start()
    everything = pltpu.make_async_remote_copy(
        src_ref=gram_r.at[pl.ds(1, total - 1)], dst_ref=gram_r.at[pl.ds(1, total - 1)],
        send_sem=gram_send, recv_sem=gram_recv,
        device_id=group_target(1), device_id_type=pl.DeviceIdType.MESH)
    everything.wait_recv()

    half = np_ * nq
    own = mine
    if half > 1:
        own = own + jnp.sum(gram_r[1:half], axis=0)
    sums = [own] + [jnp.sum(gram_r[half * e:half * (e + 1)], axis=0) for e in range(1, ne)]
    steps = []
    for e in range(ne):
        for m in range(members):
            g_rr, g_ra, g_aa, g_ab = [
                jnp.sum(jnp.where(lane_1 == 4 * m + q, sums[e], 0.0), axis=1, keepdims=True)
                for q in range(4)
            ]
            first_step = g_rr / g_ra
            following = g_rr - 2.0 * first_step * g_ra + first_step * first_step * g_aa
            growth = 1.0 + following / g_rr
            curve = (growth * growth * g_ra - 2.0 * growth * first_step * g_aa
                     + first_step * first_step * g_ab)
            second_step = following / curve
            share = 1.0 / (members * ne)
            steps.append(((first_step + second_step * growth) * share,
                          second_step * first_step * share))

    peer_part = wide_blank.at[pl.ds(0, 1 + 2 * members)]
    peer_bulk = to_peer(peer_part, peer_part)
    peer_bulk.wait_recv()
    share = 1.0 / (members * ne)

    def final_step(z, carry):
        for c in range(2):
            value = share * (w_core[c, z] + w_peer[c, z])
            for m in range(members):
                one, two = steps[m]
                value = value + one * r_core[m, c, z] - two * a_core[m, c, z]
                one, two = steps[members + m]
                value = value + one * r_peer[m, c, z] - two * a_peer[m, c, z]
            out_ref[c, z] = value
        return carry

    lax.fori_loop(0, layers, final_step, 0)

    settle(list(range(members)), False)
    peer_bulk.wait_send()
    everything.wait_send()


def body(sizes, u_prior, friction_rows, friction_table, bed_fixed, ice_mask):
    members, _, layers, rows, cols = u_prior.shape
    levels = friction_table.shape[0]
    total = sizes[0] * sizes[1] * sizes[2]
    fixed = 2 + members
    pairs = (fixed + fixed % 2 + members * 2 * layers) // 2
    fields, lanes = 2 * members + 1, 2 * cols
    rounds = max(max(sizes[0], sizes[1]) - 2, 1)
    f32 = jnp.float32
    matrices = jnp.asarray(stencils(layers, members, lanes), jnp.bfloat16)
    any_space = pl.BlockSpec(memory_space=pl.ANY)
    vmem = lambda *shape: pltpu.VMEM(shape, f32)
    core = (members, 2, layers, rows, cols)
    tall = (PAD, lanes)
    each = (members, 2) + tall
    inputs = (friction_rows, u_prior, friction_table, bed_fixed, ice_mask, matrices)
    return pl.pallas_call(
        functools.partial(kernel, sizes),
        out_shape=pltpu.VMEM((2, layers, rows, cols), f32),
        in_specs=[any_space] * 6,
        out_specs=pl.BlockSpec(memory_space=pltpu.VMEM),
        scratch_shapes=[
            pltpu.SMEM((members,), jnp.int32), vmem(fields, layers + 1, SPAN, cols),
            vmem(levels, rows, cols),
            pltpu.VMEM((rows, cols), jnp.int32), pltpu.VMEM((rows, cols), jnp.int32),
            pltpu.VMEM(matrices.shape, jnp.bfloat16),
            vmem(pairs, 8, cols), vmem(pairs, 8, cols),
            vmem(2, members + 1, 2, 8, cols), vmem(2, 2, members + 1, 8, cols),
            vmem(pairs, 8, cols), vmem(pairs, 8, cols),
            vmem(2, members + 1, 2, 8, cols), vmem(2, 2, members + 1, 8, cols),
            vmem(fields, *tall), vmem(*tall), vmem(members, *tall),
            vmem(*each), vmem(*each), vmem(*each), vmem(*each), vmem(*each),
            vmem(2 + members, TALL, lanes),
            vmem(*core[1:]), vmem(*core), vmem(*core), vmem(*core), vmem(*core), vmem(*core[1:]),
            vmem(1, 1, cols), vmem(total, 1, cols), vmem(2 * pairs + 8 * (members + 1), 8, cols),
            vmem(1 + 2 * members, *core[1:]),
            pltpu.SemaphoreType.REGULAR((rounds,)),
            pltpu.SemaphoreType.DMA((members + 5,)),
            pltpu.SemaphoreType.DMA, pltpu.SemaphoreType.DMA((members,)),
            pltpu.SemaphoreType.DMA, pltpu.SemaphoreType.DMA,
            pltpu.SemaphoreType.DMA, pltpu.SemaphoreType.DMA,
        ],
        compiler_params=pltpu.CompilerParams(
            collective_id=0, has_side_effects=True, vmem_limit_bytes=40 << 20),
        name="picard",
    )(*[pltpu.with_memory_space_constraint(x, pltpu.HBM) for x in inputs])


def solution(mesh):
    sizes = (mesh.shape["plane"], mesh.shape["planey"], mesh.shape["ens"])
    in_specs = (
        P(("group", "ens"), None, None, "plane", "planey"),
        P(("group", "ens")),
        P("group", "plane", "planey"),
        P("plane", "planey"),
        P("plane", "planey"),
    )
    out_specs = P("group", None, "plane", "planey")
    return jax.shard_map(functools.partial(body, sizes), mesh=mesh, in_specs=in_specs,
                         out_specs=out_specs, check_vma=False)
```

```python
import functools
import math
import numpy as np
import jax
import jax.numpy as jnp
from jax import lax
from jax.experimental import pallas as pl
from jax.experimental.pallas import tpu as pltpu
from jax.sharding import PartitionSpec as P

bed_unit = 2.0 ** (-29)
HALO = 4
TOP = 8
SPAN = 24
TALL = 144
PAD = 160
STEP = 16
STEP_I = (0.25, 0.125)
STEP_J = (0.125, 0.25)


def iota(shape, dim):
    return lax.broadcasted_iota(jnp.int32, shape, dim)


def turn(x, step):
    return pltpu.roll(x, step % x.shape[1], 1)


def stencils(layers, members, lanes):
    def matrix(entry):
        out = np.zeros((lanes, lanes), np.float32)
        for z in range(layers):
            for i in range(-HALO, SPAN - HALO):
                for dz in (-1, 0, 1):
                    for di in (-1, 0, 1):
                        if 0 <= z + dz < layers and -HALO <= i + di < SPAN - HALO:
                            out[(z + dz) * SPAN + (i + di) % SPAN, z * SPAN + i % SPAN] = entry(dz, di)
        return out

    def copies(slot, targets, steps):
        out = np.zeros((lanes, lanes), np.float32)
        for z in targets:
            for i in range(-HALO, SPAN - HALO):
                for di, weight in steps:
                    if -HALO <= i + di < SPAN - HALO:
                        out[slot * SPAN + (i + di) % SPAN, z * SPAN + i % SPAN] = weight
        return out

    same, difference = ((0, 1.0),), ((1, 1.0), (-1, -1.0))
    every = range(layers)
    out = [matrix(lambda dz, di, c=c: (2.0 - abs(dz)) * (STEP_I[c] if di else 1.0)) for c in range(2)]
    out.append(matrix(lambda dz, di: 0.0 if dz else float(di)))
    out.append(matrix(lambda dz, di: 0.0 if di else float(dz)))
    out += [copies(1, every, same), copies(0, every, same), copies(0, every, difference)]
    out += [copies(2 + m, (0,), same) for m in range(members)]
    return np.stack(out)


def kernel(sizes, rows_hbm, u_hbm, table_hbm, bed_hbm, mask_hbm, matrix_hbm, out_ref,
           rows_ref, flat, table_v, bed_v, mask_v, matrix,
           up_s, down_s, side_s, corner_s,
           below_r, above_r, side_r, corner_r,
           tall, cover, roots, tr, pa, pb, r_ext, a_ext, force,
           w_core, r_core, a_core, r_peer, a_peer, w_peer, gram_s, gram_r, gram_blank, blank, wide_blank,
           relay, in_sem, halo_send, halo_recv, peer_send, peer_recv, gram_send, gram_recv):
    np_, nq, ne = sizes
    members, _, layers, rows, cols = u_hbm.shape
    ix, iy, ie = lax.axis_index("plane"), lax.axis_index("planey"), lax.axis_index("ens")
    total = np_ * nq * ne
    mesh_id = pl.DeviceIdType.MESH
    fixed = 2 + members
    lanes = 2 * cols
    assert rows + 2 * HALO == SPAN and cols == 128 and layers * SPAN <= lanes and fixed <= layers
    other = 2 * members

    reach = max(np_, nq)
    rounds = reach - 2 if reach > 3 else reach - 1

    def neighbours(every_core):
        found = []
        for dx, dy in ((-1, -1), (-1, 1), (1, -1), (1, 1), (-1, 0), (1, 0), (0, -1), (0, 1), (0, 0)):
            for de in range(ne):
                if (dx, dy, de) == (0, 0, 0) or (de and (dx or dy) and not every_core):
                    continue
                tx, ty = ix + dx, iy + dy
                ok = (tx >= 0) & (tx < np_) & (ty >= 0) & (ty < nq)
                where = {"plane": jnp.clip(tx, 0, np_ - 1), "planey": jnp.clip(ty, 0, nq - 1),
                         "ens": lax.rem(ie + de, ne)}
                found.append((ok if dx or dy else None, where))
        return found

    span_x = 1 + (ix > 0).astype(jnp.int32) + (ix < np_ - 1).astype(jnp.int32)
    span_y = 1 + (iy > 0).astype(jnp.int32) + (iy < nq - 1).astype(jnp.int32)
    near_count = span_x * span_y + ne - 2
    wide_count = span_x * span_y * ne - 1

    def signal(sem, every_core):
        for ok, where in neighbours(every_core):
            def tell(where=where):
                pl.semaphore_signal(sem, inc=1, device_id=where, device_id_type=mesh_id)
            tell() if ok is None else pl.when(ok)(tell)

    barrier = pltpu.get_barrier_semaphore()
    signal(barrier, False)

    loads = [
        pltpu.make_async_copy(src, dst, in_sem.at[i])
        for i, (src, dst) in enumerate(
            [(u_hbm.at[m], flat.at[pl.ds(2 * m, 2), pl.ds(0, layers), pl.ds(0, rows)])
             for m in range(members)]
            + [(table_hbm, table_v), (bed_hbm, bed_v), (mask_hbm, mask_v), (rows_hbm, rows_ref),
               (matrix_hbm, matrix)])
    ]
    for load in loads:
        load.start()
    late = loads.pop()

    def group_place(d):
        de, rest = d // (np_ * nq), d % (np_ * nq)
        return (lax.rem(2 * np_ - 1 - ix + rest // nq, np_), lax.rem(2 * nq - 1 - iy + rest % nq, nq),
                lax.rem(ie + de, ne))

    def each_peer(fn):
        if total <= 32:
            for d in range(total):
                fn(d)
        else:
            def step(d, carry):
                fn(d)
                return carry
            lax.fori_loop(0, total, step, 0)

    planes = [[(other, k) for k in range(fixed + fixed % 2)]] + [
        [(2 * m + c, z) for z in range(layers) for c in range(2)] for m in range(members)]
    fields = [(other,)] + [(2 * m, 2 * m + 1) for m in range(members)]
    chunks = range(len(planes))
    pair_at = [sum(len(p) for p in planes[:k]) // 2 for k in chunks]
    pair_count = [len(p) // 2 for p in planes]

    has_up, has_down = ix > 0, ix < np_ - 1
    has_left, has_right = iy > 0, iy < nq - 1
    flows = [[] for _ in chunks]
    absent = []
    for dx, dy, src, dst in (
        (-1, -1, corner_s.at[0, 0], corner_r.at[1, 1]),
        (-1, 1, corner_s.at[0, 1], corner_r.at[1, 0]),
        (1, -1, corner_s.at[1, 0], corner_r.at[0, 1]),
        (1, 1, corner_s.at[1, 1], corner_r.at[0, 0]),
        (0, -1, side_s.at[0], side_r.at[1]),
        (0, 1, side_s.at[1], side_r.at[0]),
        (-1, 0, up_s, below_r),
        (1, 0, down_s, above_r),
    ):
        tx, ty = ix + dx, iy + dy
        sx, sy = ix - dx, iy - dy
        to_ok = (tx >= 0) & (tx < np_) & (ty >= 0) & (ty < nq)
        from_ok = (sx >= 0) & (sx < np_) & (sy >= 0) & (sy < nq)
        absent.append((jnp.logical_not(from_ok), dst))
        for k in chunks:
            part = pl.ds(k, 1) if dy else pl.ds(pair_at[k], pair_count[k])
            copy = pltpu.make_async_remote_copy(
                src_ref=src.at[part], dst_ref=dst.at[part],
                send_sem=halo_send, recv_sem=halo_recv.at[k],
                device_id={"plane": jnp.clip(tx, 0, np_ - 1), "planey": jnp.clip(ty, 0, nq - 1)},
                device_id_type=mesh_id)
            flows[k].append((to_ok, copy))

    def tiles(count):
        return blank.at[pl.ds(0, count)]

    def settle(chunk_list, received):
        for up in (0, 1):
            for down in (0, 1):
                for left in (0, 1):
                    for right in (0, 1):
                        if (up + down > np_ - 1 or left + right > nq - 1
                                or (np_ > 1 and up + down == 0) or (nq > 1 and left + right == 0)):
                            continue
                        count = sum(
                            pair_count[k] * (up + down) + (2 + up + down) * (left + right)
                            for k in chunk_list)
                        if count == 0:
                            continue
                        here = ((has_up == bool(up)) & (has_down == bool(down))
                                & (has_left == bool(left)) & (has_right == bool(right)))
                        bulk = pltpu.make_async_remote_copy(
                            src_ref=tiles(count), dst_ref=tiles(count), send_sem=halo_send,
                            recv_sem=halo_recv.at[chunk_list[0]],
                            device_id={"ens": lax.rem(ie + 1, ne)}, device_id_type=mesh_id)
                        pl.when(here)(bulk.wait_recv if received else bulk.wait_send)

    rim = jnp.zeros((SPAN - rows, cols), jnp.float32)
    for f in range(other + 1):
        flat[f, layers] = jnp.zeros((SPAN, cols), jnp.float32)
        for z in range(layers):
            flat[f, z, pl.ds(rows, SPAN - rows)] = rim
    for k in range(fixed, layers):
        flat[other, k, pl.ds(0, rows)] = jnp.zeros((rows, cols), jnp.float32)

    for load in loads:
        load.wait()

    cover_core = mask_v[...].astype(jnp.float32)
    flat[other, 0, pl.ds(0, rows)] = bed_v[...].astype(jnp.float32) * bed_unit
    flat[other, 1, pl.ds(0, rows)] = cover_core
    for m in range(members):
        flat[other, 2 + m, pl.ds(0, rows)] = table_v[rows_ref[m]]
    lane8 = iota((8, cols), 1)

    def places(start, offset):
        out = None
        for z in range(layers):
            low = z * SPAN + start - offset
            if -HALO < low < cols:
                here = (lane8 >= low) & (lane8 < low + HALO)
                out = here if out is None else out | here
        return out

    def stood_up(f):
        plain = flat[f].reshape((layers + 1) * SPAN, cols)
        return [plain[cols * h:cols * (h + 1)].T for h in range(2)]

    for k in chunks:
        for i, at in enumerate(planes[k]):
            half = pl.ds(HALO * (i % 2), HALO)
            up_s[pair_at[k] + i // 2, half] = flat[at + (pl.ds(0, HALO),)]
            down_s[pair_at[k] + i // 2, half] = flat[at + (pl.ds(rows - HALO, HALO),)]
        edges = []
        for f in fields[k]:
            halves = stood_up(f)
            edges.append([[half[start:start + HALO] for half in halves] for start in (0, cols - HALO)])
        if len(edges) == 1:
            edges.append([[jnp.zeros((HALO, cols), jnp.float32)] * 2] * 2)
        for h in range(2):
            pair = [jnp.concatenate([edges[0][h][q], edges[1][h][q]], axis=0) for q in range(2)]
            side_s[h, k, 0] = pair[0]
            side_s[h, k, 1] = pair[1]
            corner_s[0, h, k] = jnp.where(places(0, 0), pair[0], pair[1])
            corner_s[1, h, k] = jnp.where(places(rows - HALO, 0), pair[0], pair[1])

    pl.semaphore_wait(barrier, near_count)
    for chunk in flows:
        for to_ok, copy in chunk:
            pl.when(to_ok)(copy.start)
    if rounds > 0:
        signal(relay.at[0], False)

    for gone, dst in absent:
        @pl.when(gone)
        def _(dst=dst):
            dst[...] = jnp.zeros(dst.shape, jnp.float32)
    for c in range(2):
        for z in range(layers):
            summed = flat[c, z, pl.ds(0, rows)]
            for m in range(1, members):
                summed = summed + flat[2 * m + c, z, pl.ds(0, rows)]
            w_core[c, z] = cover_core * summed

    peer = {"ens": lax.rem(ie + 1, ne)}

    def to_peer(src, dst):
        return pltpu.make_async_remote_copy(
            src_ref=src, dst_ref=dst, send_sem=peer_send, recv_sem=peer_recv,
            device_id=peer, device_id_type=mesh_id)

    send_w = to_peer(w_core, w_peer)
    send_r = [to_peer(r_core.at[m], r_peer.at[m]) for m in range(members)]
    send_a = [to_peer(a_core.at[m], a_peer.at[m]) for m in range(members)]
    send_w.start()

    def relay_wait(k):
        pl.semaphore_wait(relay.at[k], wide_count if k else near_count)

    def relay_on(k):
        relay_wait(k - 1)
        signal(relay.at[k], True)

    if rounds > 1:
        relay_on(1)
    late.wait()

    def at(ref, index, base, count=TALL):
        return jnp.concatenate([ref[index + (q, pl.ds(base, count))] for q in range(2)], axis=1)

    def put(ref, index, base, value):
        for q in range(2):
            ref[index + (q, pl.ds(base, value.shape[0]))] = value[:, cols * q:cols * (q + 1)]

    def assemble(k):
        settle([k], True)
        for i, place in enumerate(planes[k]):
            half = pl.ds(HALO * (i % 2), HALO)
            pair = pair_at[k] + i // 2
            flat[place + (pl.ds(rows, HALO),)] = below_r[pair, half]
            flat[place + (pl.ds(rows + HALO, HALO),)] = above_r[pair, half]
        for h in range(2):
            over = turn(corner_r[0, h, k], SPAN - rows)
            under = turn(corner_r[1, h, k], rows)
            start = TOP + cols if h else TOP - HALO
            for q in range(2):
                part = jnp.where(places(rows + HALO, cols * q), over, side_r[h, k, q])
                part = jnp.where(places(rows, cols * q), under, part)
                for n, f in enumerate(fields[k]):
                    tall[f, q, pl.ds(start, HALO)] = part[HALO * n:HALO * (n + 1)]
        for f in fields[k]:
            for q, half in enumerate(stood_up(f)):
                tall[f, q, pl.ds(TOP, cols)] = half

    def times(which, count, *makers):
        parts = []
        for start in range(0, count, STEP):
            for maker in makers:
                x = maker(start)
                high = x.astype(jnp.bfloat16)
                parts += [high, (x - high.astype(jnp.float32)).astype(jnp.bfloat16)]
        lhs = jnp.concatenate(parts, axis=0)
        outs = [jnp.dot(lhs, matrix[k], preferred_element_type=jnp.float32) for k in which]

        def piece(out, start, i):
            low = 2 * (start * len(makers) + STEP * i)
            return out[low:low + STEP] + out[low + STEP:low + 2 * STEP]

        return [(start, [[piece(out, start, i) for i in range(len(makers))] for out in outs])
                for start in range(0, count, STEP)]

    root_base, res_base, img_base = TOP - 3, TOP - 2, TOP - 1
    lane = iota((8, lanes), 1)
    layer = sum([(lane >= SPAN * z).astype(jnp.int32) for z in range(1, layers + 1)])
    place = lane - SPAN * layer
    inside = ((place < rows) & (layer < layers)).astype(jnp.float32)[0:1]

    def prepare():
        put(cover, (), root_base, jnp.dot(
            at(tall, (other,), root_base).astype(jnp.bfloat16), matrix[4],
            preferred_element_type=jnp.float32))

    def prepare_force():
        b = res_base
        row = (ix * rows + jnp.where(place < rows + HALO, place, place - SPAN))[0:1]
        thickness = 1.0 + 2.0 * row.astype(jnp.float32) / (np_ * rows - 1)

        def field(start):
            return at(tall, (other,), b + start, STEP)

        def across(start):
            return at(tall, (other,), b + start + 1, STEP) - at(tall, (other,), b + start - 1, STEP)

        frictions = range(7, 7 + members)
        for (start, first), (_, second) in zip(times((6, *frictions), TALL, field), times((5,), TALL, across)):
            covered = at(cover, (), b + start, STEP)
            here = pl.ds(start, STEP)
            force[0, here] = -(covered * thickness * (first[0][0] * 0.5))
            force[1, here] = -(covered * thickness * (second[0][0] * 0.5))
            for m in range(members):
                force[2 + m, here] = (1.0 - covered) + covered * first[1 + m][0]

    def roots_level(m):
        b = root_base

        def u(start, shift=0):
            return at(tall, (2 * m,), b + start + shift, STEP)

        def v(start, shift=0):
            return at(tall, (2 * m + 1,), b + start + shift, STEP)

        for start, ((u_i, v_i), (u_z, v_z)) in times((2, 3), TALL, u, v):
            u_j, v_j = u(start, 1) - u(start, -1), v(start, 1) - v(start, -1)
            shear = u_j + v_i
            strain = (4.0 * (u_i * (u_i + v_j) + v_j * v_j) + shear * shear
                      + (u_z * u_z + v_z * v_z)) * 0.0625
            root = at(cover, (), b + start, STEP) * jnp.exp(
                jnp.log(strain + 0.1) * (-1.0 / 6.0) + 0.5 * math.log(2.0))
            put(roots, (m,), b + start, root)
            put(pa, (m, 0), b + start, root * u(start))
            put(pa, (m, 1), b + start, root * v(start))

    def leaning(ref, index, base, c):
        def maker(start):
            low = base + start
            return at(ref, index, low, STEP) + STEP_J[c] * (
                at(ref, index, low - 1, STEP) + at(ref, index, low + 1, STEP))
        return maker

    def residual_level(m):
        b = res_base
        for c in range(2):
            for start, ((near, moved),) in times(
                    (c,), TALL, leaning(roots, (m,), b, c), leaning(pa, (m, c), b, c)):
                low, here = b + start, pl.ds(start, STEP)
                root = at(roots, (m,), low, STEP)
                weight = root * near + force[2 + m, here]
                r = force[c, here] - (weight * (at(cover, (), low, STEP) * at(tall, (2 * m + c,), low, STEP))
                                      - root * moved)
                put(tr, (m, c), low, weight)
                put(r_ext, (m, c), low, r)
                put(pb, (m, c), low, root * r)

    def image_level(m):
        b = img_base
        for c in range(2):
            for start, ((moved,),) in times((c,), TALL, leaning(pb, (m, c), b, c)):
                low = b + start
                root = at(roots, (m,), low, STEP)
                a = at(tr, (m, c), low, STEP) * at(r_ext, (m, c), low, STEP) - root * moved
                put(a_ext, (m, c), low, a)
                put(pa, (m, c), low, root * a)

    def second_level(m):
        sums = None
        for c in range(2):
            def scaled(start):
                return at(pa, (m, c), TOP + start, STEP)

            def one_way(start):
                return scaled(start) + (2.0 * STEP_J[c]) * at(pa, (m, c), TOP - 1 + start, STEP)

            for start, ((out,),) in times((c,), cols, one_way):
                low = TOP + start
                r, a = at(r_ext, (m, c), low, STEP), at(a_ext, (m, c), low, STEP)
                square = a * a
                terms = (r * r, r * a, square, at(tr, (m, c), low, STEP) * square - scaled(start) * out)
                sums = terms if sums is None else [s + t for s, t in zip(sums, terms)]
        return [inside * jnp.sum(s, axis=0, keepdims=True) for s in sums]

    grams = []
    assemble(0)
    prepare()
    prepare_force()
    for m in range(members):
        assemble(1 + m)
        roots_level(m)
        if m > 0:
            image_level(m - 1)
        residual_level(m)
        if m > 0:
            grams.append(second_level(m - 1))
        if m == 0:
            for k in range(2, rounds):
                relay_on(k)
    image_level(members - 1)
    grams.append(second_level(members - 1))

    lane_1 = iota((1, cols), 1)
    mine = jnp.zeros((1, cols), jnp.float32)
    for m in range(members):
        for q, acc in enumerate(grams[m]):
            mine = jnp.where(lane_1 == 4 * m + q, jnp.sum(acc, axis=1, keepdims=True), mine)
    gram_s[0] = mine

    if rounds > 0:
        relay_wait(rounds - 1)

    def send_gram(d):
        px, py, pe = group_place(d)
        copy = pltpu.make_async_remote_copy(
            src_ref=gram_s, dst_ref=gram_r.at[pl.ds(d, 1)],
            send_sem=gram_send, recv_sem=gram_recv,
            device_id={"plane": px, "planey": py, "ens": pe}, device_id_type=mesh_id)
        own = (px == ix) & (py == iy) & (pe == ie)
        pl.when(jnp.logical_not(own))(copy.start)

    each_peer(send_gram)
    own_place = lax.rem(2 * ix + 1, np_) * nq + lax.rem(2 * iy + 1, nq)
    gram_r[pl.ds(own_place, 1)] = mine[None]

    def lie_down(src, dst):
        for c in range(2):
            flat_rows = jnp.concatenate(
                [src[c, q, pl.ds(TOP, cols)].T for q in range(2)], axis=0)
            for z in range(layers):
                dst[c, z] = flat_rows[SPAN * z:SPAN * z + rows]

    for m in range(members):
        lie_down(r_ext.at[m], r_core.at[m])
        send_r[m].start()
        lie_down(a_ext.at[m], a_core.at[m])
        send_a[m].start()
    everything = pltpu.make_async_remote_copy(
        src_ref=gram_blank, dst_ref=gram_blank, send_sem=gram_send, recv_sem=gram_recv,
        device_id=peer, device_id_type=mesh_id)
    everything.wait_recv()

    half = np_ * nq
    sums = [jnp.sum(gram_r[half * e:half * (e + 1)], axis=0) for e in range(ne)]
    steps = []
    for e in range(ne):
        for m in range(members):
            g_rr, g_ra, g_aa, g_ab = [
                jnp.sum(jnp.where(lane_1 == 4 * m + q, sums[e], 0.0), axis=1, keepdims=True)
                for q in range(4)
            ]
            first_step = g_rr / g_ra
            following = g_rr - 2.0 * first_step * g_ra + first_step * first_step * g_aa
            growth = 1.0 + following / g_rr
            curve = (growth * growth * g_ra - 2.0 * growth * first_step * g_aa
                     + first_step * first_step * g_ab)
            second_step = following / curve
            share = 1.0 / (members * ne)
            steps.append(((first_step + second_step * growth) * share,
                          second_step * first_step * share))

    peer_part = wide_blank.at[pl.ds(0, 1 + 2 * members)]
    peer_bulk = to_peer(peer_part, peer_part)
    peer_bulk.wait_recv()
    share = 1.0 / (members * ne)

    def final_step(z, carry):
        for c in range(2):
            value = share * (w_core[c, z] + w_peer[c, z])
            for m in range(members):
                one, two = steps[m]
                value = value + one * r_core[m, c, z] - two * a_core[m, c, z]
                one, two = steps[members + m]
                value = value + one * r_peer[m, c, z] - two * a_peer[m, c, z]
            out_ref[c, z] = value
        return carry

    lax.fori_loop(0, layers, final_step, 0)

    settle(list(chunks), False)
    peer_bulk.wait_send()
    everything.wait_send()


def body(sizes, u_prior, friction_rows, friction_table, bed_fixed, ice_mask):
    members, _, layers, rows, cols = u_prior.shape
    levels = friction_table.shape[0]
    total = sizes[0] * sizes[1] * sizes[2]
    fixed = 2 + members
    pairs = (fixed + fixed % 2 + members * 2 * layers) // 2
    fields, lanes = 2 * members + 1, 2 * cols
    rounds = max(max(sizes[0], sizes[1]) - 2, 2)
    f32 = jnp.float32
    matrices = jnp.asarray(stencils(layers, members, lanes), jnp.bfloat16)
    any_space = pl.BlockSpec(memory_space=pl.ANY)
    vmem = lambda *shape: pltpu.VMEM(shape, f32)
    core = (members, 2, layers, rows, cols)
    tall = (2, PAD, cols)
    each = (members, 2) + tall
    inputs = (friction_rows, u_prior, friction_table, bed_fixed, ice_mask, matrices)
    return pl.pallas_call(
        functools.partial(kernel, sizes),
        out_shape=pltpu.VMEM((2, layers, rows, cols), f32),
        in_specs=[any_space] * 6,
        out_specs=pl.BlockSpec(memory_space=pltpu.VMEM),
        scratch_shapes=[
            pltpu.SMEM((members,), jnp.int32), vmem(fields, layers + 1, SPAN, cols),
            vmem(levels, rows, cols),
            pltpu.VMEM((rows, cols), jnp.int32), pltpu.VMEM((rows, cols), jnp.int32),
            pltpu.VMEM(matrices.shape, jnp.bfloat16),
            vmem(pairs, 8, cols), vmem(pairs, 8, cols),
            vmem(2, members + 1, 2, 8, cols), vmem(2, 2, members + 1, 8, cols),
            vmem(pairs, 8, cols), vmem(pairs, 8, cols),
            vmem(2, members + 1, 2, 8, cols), vmem(2, 2, members + 1, 8, cols),
            vmem(fields, *tall), vmem(*tall), vmem(members, *tall),
            vmem(*each), vmem(*each), vmem(*each), vmem(*each), vmem(*each),
            vmem(2 + members, TALL, lanes),
            vmem(*core[1:]), vmem(*core), vmem(*core), vmem(*core), vmem(*core), vmem(*core[1:]),
            vmem(1, 1, cols), vmem(total, 1, cols), vmem(total - 1, 1, cols), vmem(2 * pairs + 8 * (members + 1), 8, cols),
            vmem(1 + 2 * members, *core[1:]),
            pltpu.SemaphoreType.REGULAR((rounds,)),
            pltpu.SemaphoreType.DMA((members + 5,)),
            pltpu.SemaphoreType.DMA, pltpu.SemaphoreType.DMA((members + 1,)),
            pltpu.SemaphoreType.DMA, pltpu.SemaphoreType.DMA,
            pltpu.SemaphoreType.DMA, pltpu.SemaphoreType.DMA,
        ],
        compiler_params=pltpu.CompilerParams(
            collective_id=0, has_side_effects=True, vmem_limit_bytes=40 << 20),
        name="picard",
    )(*[pltpu.with_memory_space_constraint(x, pltpu.HBM) for x in inputs])


def solution(mesh):
    sizes = (mesh.shape["plane"], mesh.shape["planey"], mesh.shape["ens"])
    in_specs = (
        P(("group", "ens"), None, None, "plane", "planey"),
        P(("group", "ens")),
        P("group", "plane", "planey"),
        P("plane", "planey"),
        P("plane", "planey"),
    )
    out_specs = P("group", None, "plane", "planey")
    return jax.shard_map(functools.partial(body, sizes), mesh=mesh, in_specs=in_specs,
                         out_specs=out_specs, check_vma=False)
```

```python
import functools
import math
import numpy as np
import jax
import jax.numpy as jnp
from jax import lax
from jax.experimental import pallas as pl
from jax.experimental.pallas import tpu as pltpu
from jax.sharding import PartitionSpec as P

bed_unit = 2.0 ** (-29)
HALO = 4
TOP = 8
SPAN = 24
TALL = 144
PAD = 160
STEP = 16
STEP_I = (0.25, 0.125)
STEP_J = (0.125, 0.25)


def iota(shape, dim):
    return lax.broadcasted_iota(jnp.int32, shape, dim)


def turn(x, step):
    return pltpu.roll(x, step % x.shape[1], 1)


def stencils(layers, lanes):
    def matrix(entry):
        out = np.zeros((lanes, lanes), np.float32)
        for z in range(layers):
            for i in range(-HALO, SPAN - HALO):
                for dz in (-1, 0, 1):
                    for di in (-1, 0, 1):
                        if 0 <= z + dz < layers and -HALO <= i + di < SPAN - HALO:
                            out[(z + dz) * SPAN + (i + di) % SPAN, z * SPAN + i % SPAN] = entry(dz, di)
        return out

    def copies(slot, targets, steps):
        out = np.zeros((lanes, lanes), np.float32)
        for z in targets:
            for i in range(-HALO, SPAN - HALO):
                for di, weight in steps:
                    if -HALO <= i + di < SPAN - HALO:
                        out[slot * SPAN + (i + di) % SPAN, z * SPAN + i % SPAN] = weight
        return out

    same, difference = ((0, 1.0),), ((1, 1.0), (-1, -1.0))
    every = range(layers)
    out = [matrix(lambda dz, di, c=c: (2.0 - abs(dz)) * (STEP_I[c] if di else 1.0)) for c in range(2)]
    out.append(matrix(lambda dz, di: 0.0 if dz else float(di)))
    out += [copies(1, every, same), copies(0, every, same), copies(0, every, difference)]
    return np.stack(out)


def kernel(sizes, rows_hbm, u_hbm, table_hbm, bed_hbm, mask_hbm, matrix_hbm, out_ref,
           rows_ref, flat, table_v, bed_v, mask_v, matrix,
           up_s, down_s, side_s, corner_s,
           below_r, above_r, side_r, corner_r,
           steep, tall, tall_steep, cover, roots, tr, pa, pb, r_ext, a_ext, force,
           w_core, r_core, a_core, r_peer, a_peer, w_peer, gram_s, gram_r, gram_blank, blank, wide_blank,
           relay, in_sem, halo_recv, peer_recv, gram_recv):
    np_, nq, ne = sizes
    other, layers, rows, cols = u_hbm.shape
    members = other // 2
    ix, iy, ie = lax.axis_index("plane"), lax.axis_index("planey"), lax.axis_index("ens")
    total = np_ * nq * ne
    mesh_id = pl.DeviceIdType.MESH
    fixed = 2 + members
    lanes = 2 * cols
    assert rows + 2 * HALO == SPAN and cols == 128 and layers * SPAN <= lanes
    assert fixed <= layers and fixed * SPAN <= cols
    halo_send, peer_send, gram_send = in_sem.at[0], in_sem.at[1], in_sem.at[2]

    reach = max(np_, nq)
    rounds = reach - 2 if reach > 3 else reach - 1

    def neighbours(every_core):
        found = []
        for dx, dy in ((-1, -1), (-1, 1), (1, -1), (1, 1), (-1, 0), (1, 0), (0, -1), (0, 1), (0, 0)):
            for de in range(ne):
                if (dx, dy, de) == (0, 0, 0) or (de and (dx or dy) and not every_core):
                    continue
                tx, ty = ix + dx, iy + dy
                ok = (tx >= 0) & (tx < np_) & (ty >= 0) & (ty < nq)
                where = {"plane": jnp.clip(tx, 0, np_ - 1), "planey": jnp.clip(ty, 0, nq - 1),
                         "ens": lax.rem(ie + de, ne)}
                found.append((ok if dx or dy else None, where))
        return found

    span_x = 1 + (ix > 0).astype(jnp.int32) + (ix < np_ - 1).astype(jnp.int32)
    span_y = 1 + (iy > 0).astype(jnp.int32) + (iy < nq - 1).astype(jnp.int32)
    near_count = span_x * span_y + ne - 2
    wide_count = span_x * span_y * ne - 1

    def signal(sem, every_core):
        for ok, where in neighbours(every_core):
            def tell(where=where):
                pl.semaphore_signal(sem, inc=1, device_id=where, device_id_type=mesh_id)
            tell() if ok is None else pl.when(ok)(tell)

    barrier = pltpu.get_barrier_semaphore()
    signal(barrier, False)

    loads = [
        pltpu.make_async_copy(src, dst, in_sem.at[i])
        for i, (src, dst) in enumerate(
            ((u_hbm, flat.at[pl.ds(0, other), pl.ds(0, layers), pl.ds(0, rows)]),
             (table_hbm, table_v), (bed_hbm, bed_v), (mask_hbm, mask_v), (rows_hbm, rows_ref),
             (matrix_hbm, matrix)))
    ]
    for load in loads:
        load.start()
    late = loads.pop()

    def group_place(d):
        de, rest = d // (np_ * nq), d % (np_ * nq)
        return (lax.rem(2 * np_ - 1 - ix + rest // nq, np_), lax.rem(2 * nq - 1 - iy + rest % nq, nq),
                lax.rem(ie + de, ne))

    def each_peer(fn):
        if total <= 32:
            for d in range(total):
                fn(d)
        else:
            def step(d, carry):
                fn(d)
                return carry
            lax.fori_loop(0, total, step, 0)

    planes = [[(other, k) for k in range(fixed + fixed % 2)]] + [
        [(2 * m + c, z) for z in range(layers) for c in range(2)] for m in range(members)]
    fields = [(other,)] + [(2 * m, 2 * m + 1) for m in range(members)]
    chunks = range(len(planes))
    pair_at = [sum(len(p) for p in planes[:k]) // 2 for k in chunks]
    pair_count = [len(p) // 2 for p in planes]

    has_up, has_down = ix > 0, ix < np_ - 1
    has_left, has_right = iy > 0, iy < nq - 1
    flows = [[] for _ in chunks]
    absent = []
    for dx, dy, src, dst in (
        (-1, -1, corner_s.at[0, 0], corner_r.at[1, 1]),
        (-1, 1, corner_s.at[0, 1], corner_r.at[1, 0]),
        (1, -1, corner_s.at[1, 0], corner_r.at[0, 1]),
        (1, 1, corner_s.at[1, 1], corner_r.at[0, 0]),
        (0, -1, side_s.at[0], side_r.at[1]),
        (0, 1, side_s.at[1], side_r.at[0]),
        (-1, 0, up_s, below_r),
        (1, 0, down_s, above_r),
    ):
        tx, ty = ix + dx, iy + dy
        sx, sy = ix - dx, iy - dy
        to_ok = (tx >= 0) & (tx < np_) & (ty >= 0) & (ty < nq)
        from_ok = (sx >= 0) & (sx < np_) & (sy >= 0) & (sy < nq)
        absent.append((jnp.logical_not(from_ok), dst))
        for k in chunks:
            part = pl.ds(k, 1) if dy else pl.ds(pair_at[k], pair_count[k])
            copy = pltpu.make_async_remote_copy(
                src_ref=src.at[part], dst_ref=dst.at[part],
                send_sem=halo_send, recv_sem=halo_recv.at[k],
                device_id={"plane": jnp.clip(tx, 0, np_ - 1), "planey": jnp.clip(ty, 0, nq - 1)},
                device_id_type=mesh_id)
            flows[k].append((to_ok, copy))

    def tiles(count):
        return blank.at[pl.ds(0, count)]

    def settle(chunk_list, received):
        for up in (0, 1):
            for down in (0, 1):
                for left in (0, 1):
                    for right in (0, 1):
                        if (up + down > np_ - 1 or left + right > nq - 1
                                or (np_ > 1 and up + down == 0) or (nq > 1 and left + right == 0)):
                            continue
                        count = sum(
                            pair_count[k] * (up + down) + (2 + up + down) * (left + right)
                            for k in chunk_list)
                        if count == 0:
                            continue
                        here = ((has_up == bool(up)) & (has_down == bool(down))
                                & (has_left == bool(left)) & (has_right == bool(right)))
                        bulk = pltpu.make_async_remote_copy(
                            src_ref=tiles(count), dst_ref=tiles(count), send_sem=halo_send,
                            recv_sem=halo_recv.at[chunk_list[0]],
                            device_id={"ens": lax.rem(ie + 1, ne)}, device_id_type=mesh_id)
                        pl.when(here)(bulk.wait_recv if received else bulk.wait_send)

    rim = jnp.zeros((SPAN - rows, cols), jnp.float32)
    for f in range(other + 1):
        flat[f, layers] = jnp.zeros((SPAN, cols), jnp.float32)
        for z in range(layers):
            flat[f, z, pl.ds(rows, SPAN - rows)] = rim
    for k in range(fixed, layers):
        flat[other, k, pl.ds(0, rows)] = jnp.zeros((rows, cols), jnp.float32)

    for load in loads:
        load.wait()

    cover_core = mask_v[...].astype(jnp.float32)
    flat[other, 0, pl.ds(0, rows)] = bed_v[...].astype(jnp.float32) * bed_unit
    flat[other, 1, pl.ds(0, rows)] = cover_core
    for m in range(members):
        flat[other, 2 + m, pl.ds(0, rows)] = table_v[rows_ref[m]]
    lane8 = iota((8, cols), 1)

    def places(start, offset):
        out = None
        for z in range(layers):
            low = z * SPAN + start - offset
            if -HALO < low < cols:
                here = (lane8 >= low) & (lane8 < low + HALO)
                out = here if out is None else out | here
        return out

    def stood_up(field):
        plain = field[...].reshape((layers + 1) * SPAN, cols)
        return [plain[cols * h:cols * (h + 1)].T for h in range(2)]

    def pack(k):
        for i, at in enumerate(planes[k]):
            half = pl.ds(HALO * (i % 2), HALO)
            up_s[pair_at[k] + i // 2, half] = flat[at + (pl.ds(0, HALO),)]
            down_s[pair_at[k] + i // 2, half] = flat[at + (pl.ds(rows - HALO, HALO),)]
        edges = []
        for f in fields[k]:
            halves = stood_up(flat.at[f])
            edges.append([[half[start:start + HALO] for half in halves] for start in (0, cols - HALO)])
        if len(edges) == 1:
            edges.append([[jnp.zeros((HALO, cols), jnp.float32)] * 2] * 2)
        for h in range(2):
            pair = [jnp.concatenate([edges[0][h][q], edges[1][h][q]], axis=0) for q in range(2)]
            side_s[h, k, 0] = pair[0]
            side_s[h, k, 1] = pair[1]
            corner_s[0, h, k] = jnp.where(places(0, 0), pair[0], pair[1])
            corner_s[1, h, k] = jnp.where(places(rows - HALO, 0), pair[0], pair[1])

    def send(k):
        for to_ok, copy in flows[k]:
            pl.when(to_ok)(copy.start)

    pack(0)
    pack(1)
    pl.semaphore_wait(barrier, near_count)
    send(0)
    send(1)
    for k in chunks[2:]:
        pack(k)
        send(k)
    if rounds > 0:
        signal(relay.at[0], False)

    for gone, dst in absent:
        @pl.when(gone)
        def _(dst=dst):
            dst[...] = jnp.zeros(dst.shape, jnp.float32)
    for c in range(2):
        for z in range(layers):
            summed = flat[c, z, pl.ds(0, rows)]
            for m in range(1, members):
                summed = summed + flat[2 * m + c, z, pl.ds(0, rows)]
            w_core[c, z] = cover_core * summed

    peer = {"ens": lax.rem(ie + 1, ne)}

    def to_peer(src, dst):
        return pltpu.make_async_remote_copy(
            src_ref=src, dst_ref=dst, send_sem=peer_send, recv_sem=peer_recv,
            device_id=peer, device_id_type=mesh_id)

    send_w = to_peer(w_core, w_peer)
    send_r = [to_peer(r_core.at[m], r_peer.at[m]) for m in range(members)]
    send_a = [to_peer(a_core.at[m], a_peer.at[m]) for m in range(members)]
    send_w.start()

    def relay_wait(k):
        pl.semaphore_wait(relay.at[k], wide_count if k else near_count)

    def relay_on(k):
        relay_wait(k - 1)
        signal(relay.at[k], True)

    if rounds > 1:
        relay_on(1)
    late.wait()

    def at(ref, index, base, count=TALL):
        return jnp.concatenate([ref[index + (q, pl.ds(base, count))] for q in range(2)], axis=1)

    def put(ref, index, base, value):
        for q in range(2):
            ref[index + (q, pl.ds(base, value.shape[0]))] = value[:, cols * q:cols * (q + 1)]

    def steepen(m, part):
        for z in range(layers):
            square = None
            for f in (2 * m, 2 * m + 1):
                change = None
                if z < layers - 1:
                    change = flat[f, z + 1, part]
                if z > 0:
                    change = flat[f, z - 1, part] if change is None else change - flat[f, z - 1, part]
                square = change * change if square is None else square + change * change
            steep[m, z, part] = square

    for m in range(members):
        steep[m, layers] = jnp.zeros((SPAN, cols), jnp.float32)
        steepen(m, pl.ds(0, rows))

    def assemble(k):
        for i, place in enumerate(planes[k]):
            half = pl.ds(HALO * (i % 2), HALO)
            pair = pair_at[k] + i // 2
            flat[place + (pl.ds(rows, HALO),)] = below_r[pair, half]
            flat[place + (pl.ds(rows + HALO, HALO),)] = above_r[pair, half]
        for h in range(2):
            over = turn(corner_r[0, h, k], SPAN - rows)
            under = turn(corner_r[1, h, k], rows)
            start = TOP + cols if h else TOP - HALO
            parts = []
            for q in range(2):
                part = jnp.where(places(rows + HALO, cols * q), over, side_r[h, k, q])
                part = jnp.where(places(rows, cols * q), under, part)
                for n, f in enumerate(fields[k]):
                    tall[f, q, pl.ds(start, HALO)] = part[HALO * n:HALO * (n + 1)]
                parts.append(part)
            if k:
                uppers, lowers = [turn(p, -SPAN) for p in parts], [turn(p, SPAN) for p in parts]
                for q in range(2):
                    whole = lane8 + cols * q
                    upper = jnp.where(lane8 < cols - SPAN, uppers[q], uppers[1 - q])
                    lower = jnp.where(lane8 >= SPAN, lowers[q], lowers[1 - q])
                    change = (jnp.where(whole < (layers - 1) * SPAN, upper, 0.0)
                              - jnp.where(whole >= SPAN, lower, 0.0))
                    change = change * change
                    tall_steep[k - 1, q, pl.ds(start, HALO)] = change[0:HALO] + change[HALO:2 * HALO]
        for f in fields[k]:
            for q, half in enumerate(stood_up(flat.at[f])):
                tall[f, q, pl.ds(TOP, cols)] = half
        if k:
            steepen(k - 1, pl.ds(rows, SPAN - rows))
            for q, half in enumerate(stood_up(steep.at[k - 1])):
                tall_steep[k - 1, q, pl.ds(TOP, cols)] = half

    def times(which, count, *makers):
        parts = []
        for start in range(0, count, STEP):
            for maker in makers:
                x = maker(start)
                high = x.astype(jnp.bfloat16)
                parts += [high, (x - high.astype(jnp.float32)).astype(jnp.bfloat16)]
        lhs = jnp.concatenate(parts, axis=0)
        outs = [jnp.dot(lhs, matrix[k], preferred_element_type=jnp.float32) for k in which]

        def piece(out, start, i):
            low = 2 * (start * len(makers) + STEP * i)
            return out[low:low + STEP] + out[low + STEP:low + 2 * STEP]

        return [(start, [[piece(out, start, i) for i in range(len(makers))] for out in outs])
                for start in range(0, count, STEP)]

    root_base, res_base, img_base = TOP - 3, TOP - 2, TOP - 1
    lane = iota((8, lanes), 1)
    layer = sum([(lane >= SPAN * z).astype(jnp.int32) for z in range(1, layers + 1)])
    place = lane - SPAN * layer
    inside = ((place < rows) & (layer < layers)).astype(jnp.float32)[0:1]

    def prepare():
        put(cover, (), root_base, jnp.dot(
            at(tall, (other,), root_base).astype(jnp.bfloat16), matrix[3],
            preferred_element_type=jnp.float32))

    def prepare_force():
        b = res_base
        row = (ix * rows + jnp.where(place < rows + HALO, place, place - SPAN))[0:1]
        thickness = 1.0 + 2.0 * row.astype(jnp.float32) / (np_ * rows - 1)

        def field(start):
            return at(tall, (other,), b + start, STEP)

        def across(start):
            return at(tall, (other,), b + start + 1, STEP) - at(tall, (other,), b + start - 1, STEP)

        firsts, seconds = times((5,), TALL, field), times((4,), TALL, across)
        ground = iota((STEP, cols), 1) < SPAN
        yield
        for (start, first), (_, second) in zip(firsts, seconds):
            covered = at(cover, (), b + start, STEP)
            here = pl.ds(start, STEP)
            force[0, here] = -(covered * thickness * (first[0][0] * 0.5))
            force[1, here] = -(covered * thickness * (second[0][0] * 0.5))
            for m in range(members):
                rub = turn(tall[other, 0, pl.ds(b + start, STEP)], -SPAN * (2 + m))
                rub = jnp.where(ground, covered[:, 0:cols] * rub, 0.0)
                dry = 1.0 - covered
                force[2 + m, here] = jnp.concatenate([dry[:, 0:cols] + rub, dry[:, cols:]], axis=1)
            yield

    def roots_level(m):
        b = root_base

        def u(start, shift=0):
            return at(tall, (2 * m,), b + start + shift, STEP)

        def v(start, shift=0):
            return at(tall, (2 * m + 1,), b + start + shift, STEP)

        products = times((2,), TALL, u, v)
        yield
        for start, ((u_i, v_i),) in products:
            u_j, v_j = u(start, 1) - u(start, -1), v(start, 1) - v(start, -1)
            shear = u_j + v_i
            strain = (4.0 * (u_i * (u_i + v_j) + v_j * v_j) + shear * shear
                      + at(tall_steep, (m,), b + start, STEP)) * 0.0625
            root = at(cover, (), b + start, STEP) * jnp.exp(
                jnp.log(strain + 0.1) * (-1.0 / 6.0) + 0.5 * math.log(2.0))
            put(roots, (m,), b + start, root)
            put(pa, (m, 0), b + start, root * u(start))
            put(pa, (m, 1), b + start, root * v(start))
            yield

    def leaning(ref, index, base, c):
        def maker(start):
            low = base + start
            return at(ref, index, low, STEP) + STEP_J[c] * (
                at(ref, index, low - 1, STEP) + at(ref, index, low + 1, STEP))
        return maker

    def residual_level(m):
        b = res_base
        products = []
        for c in range(2):
            products.append(times((c,), TALL, leaning(roots, (m,), b, c), leaning(pa, (m, c), b, c)))
            yield
        for steps_of in zip(*products):
            for c, (start, ((near, moved),)) in enumerate(steps_of):
                low, here = b + start, pl.ds(start, STEP)
                root = at(roots, (m,), low, STEP)
                weight = root * near + force[2 + m, here]
                r = force[c, here] - (weight * (at(cover, (), low, STEP) * at(tall, (2 * m + c,), low, STEP))
                                      - root * moved)
                put(tr, (m, c), low, weight)
                put(r_ext, (m, c), low, r)
                put(pb, (m, c), low, root * r)
            yield

    def image_level(m):
        b = img_base
        products = []
        for c in range(2):
            products.append(times((c,), TALL, leaning(pb, (m, c), b, c)))
            yield
        for steps_of in zip(*products):
            for c, (start, ((moved,),)) in enumerate(steps_of):
                low = b + start
                root = at(roots, (m,), low, STEP)
                a = at(tr, (m, c), low, STEP) * at(r_ext, (m, c), low, STEP) - root * moved
                put(a_ext, (m, c), low, a)
                put(pa, (m, c), low, root * a)
            yield

    grams = [None] * members

    def second_level(m):
        def one_way(c):
            def maker(start):
                low = TOP + start
                return at(pa, (m, c), low, STEP) + (2.0 * STEP_J[c]) * at(pa, (m, c), low - 1, STEP)
            return maker

        products = []
        for c in range(2):
            products.append(times((c,), cols, one_way(c)))
            yield
        sums = None
        for steps_of in zip(*products):
            for c, (start, ((out,),)) in enumerate(steps_of):
                low = TOP + start
                r, a = at(r_ext, (m, c), low, STEP), at(a_ext, (m, c), low, STEP)
                square = a * a
                terms = (r * r, r * a, square,
                         at(tr, (m, c), low, STEP) * square - at(pa, (m, c), low, STEP) * out)
                sums = terms if sums is None else [s + t for s, t in zip(sums, terms)]
            yield
        grams[m] = [inside * jnp.sum(s, axis=0, keepdims=True) for s in sums]

    def together(*levels):
        levels = list(levels)
        while levels:
            for level in list(levels):
                try:
                    next(level)
                except StopIteration:
                    levels.remove(level)

    settle([0], True)
    settle([1], True)
    assemble(0)
    assemble(1)
    prepare()
    together(roots_level(0), prepare_force())
    for k in range(2, rounds):
        relay_on(k)
    stages = (roots_level, residual_level, image_level, second_level)
    for turn_of in range(1, members + len(stages) - 1):
        if turn_of < members:
            settle([1 + turn_of], True)
            assemble(1 + turn_of)
        together(*[stages[turn_of - m](m) for m in range(members) if 0 <= turn_of - m < len(stages)])

    lane_1 = iota((1, cols), 1)
    mine = jnp.zeros((1, cols), jnp.float32)
    for m in range(members):
        for q, acc in enumerate(grams[m]):
            mine = jnp.where(lane_1 == 4 * m + q, jnp.sum(acc, axis=1, keepdims=True), mine)
    gram_s[0] = mine

    if rounds > 0:
        relay_wait(rounds - 1)

    def send_gram(d):
        px, py, pe = group_place(d)
        copy = pltpu.make_async_remote_copy(
            src_ref=gram_s, dst_ref=gram_r.at[pl.ds(d, 1)],
            send_sem=gram_send, recv_sem=gram_recv,
            device_id={"plane": px, "planey": py, "ens": pe}, device_id_type=mesh_id)
        own = (px == ix) & (py == iy) & (pe == ie)
        pl.when(jnp.logical_not(own))(copy.start)

    each_peer(send_gram)
    own_place = lax.rem(2 * ix + 1, np_) * nq + lax.rem(2 * iy + 1, nq)
    gram_r[pl.ds(own_place, 1)] = mine[None]

    def lie_down(src, dst):
        for c in range(2):
            flat_rows = jnp.concatenate(
                [src[c, q, pl.ds(TOP, cols)].T for q in range(2)], axis=0)
            for z in range(layers):
                dst[c, z] = flat_rows[SPAN * z:SPAN * z + rows]

    for m in range(members):
        lie_down(r_ext.at[m], r_core.at[m])
        send_r[m].start()
        lie_down(a_ext.at[m], a_core.at[m])
        send_a[m].start()
    everything = pltpu.make_async_remote_copy(
        src_ref=gram_blank, dst_ref=gram_blank, send_sem=gram_send, recv_sem=gram_recv,
        device_id=peer, device_id_type=mesh_id)
    everything.wait_recv()

    half = np_ * nq
    sums = [jnp.sum(gram_r[half * e:half * (e + 1)], axis=0) for e in range(ne)]
    steps = []
    for e in range(ne):
        for m in range(members):
            g_rr, g_ra, g_aa, g_ab = [
                jnp.sum(jnp.where(lane_1 == 4 * m + q, sums[e], 0.0), axis=1, keepdims=True)
                for q in range(4)
            ]
            first_step = g_rr / g_ra
            following = g_rr - 2.0 * first_step * g_ra + first_step * first_step * g_aa
            growth = 1.0 + following / g_rr
            curve = (growth * growth * g_ra - 2.0 * growth * first_step * g_aa
                     + first_step * first_step * g_ab)
            second_step = following / curve
            share = 1.0 / (members * ne)
            steps.append(((first_step + second_step * growth) * share,
                          second_step * first_step * share))

    peer_part = wide_blank.at[pl.ds(0, 1 + 2 * members)]
    peer_bulk = to_peer(peer_part, peer_part)
    peer_bulk.wait_recv()
    share = 1.0 / (members * ne)

    def final_step(z):
        for c in range(2):
            value = share * (w_core[c, z] + w_peer[c, z])
            for m in range(members):
                one, two = steps[m]
                value = value + one * r_core[m, c, z] - two * a_core[m, c, z]
                one, two = steps[members + m]
                value = value + one * r_peer[m, c, z] - two * a_peer[m, c, z]
            out_ref[c, z] = value

    for z in range(layers):
        final_step(z)

    settle(list(chunks), False)
    peer_bulk.wait_send()
    everything.wait_send()


def body(sizes, u_prior, friction_rows, friction_table, bed_fixed, ice_mask):
    members, _, layers, rows, cols = u_prior.shape
    levels = friction_table.shape[0]
    total = sizes[0] * sizes[1] * sizes[2]
    fixed = 2 + members
    pairs = (fixed + fixed % 2 + members * 2 * layers) // 2
    fields, lanes = 2 * members + 1, 2 * cols
    rounds = max(max(sizes[0], sizes[1]) - 2, 2)
    f32 = jnp.float32
    matrices = jnp.asarray(stencils(layers, lanes), jnp.bfloat16)
    any_space = pl.BlockSpec(memory_space=pl.ANY)
    vmem = lambda *shape: pltpu.VMEM(shape, f32)
    core = (members, 2, layers, rows, cols)
    tall = (2, PAD, cols)
    each = (members, 2) + tall
    inputs = (friction_rows, u_prior.reshape((-1,) + u_prior.shape[2:]), friction_table, bed_fixed, ice_mask, matrices)
    return pl.pallas_call(
        functools.partial(kernel, sizes),
        out_shape=pltpu.VMEM((2, layers, rows, cols), f32),
        in_specs=[any_space] * 6,
        out_specs=pl.BlockSpec(memory_space=pltpu.VMEM),
        scratch_shapes=[
            pltpu.SMEM((members,), jnp.int32), vmem(fields, layers + 1, SPAN, cols),
            vmem(levels, rows, cols),
            pltpu.VMEM((rows, cols), jnp.int32), pltpu.VMEM((rows, cols), jnp.int32),
            pltpu.VMEM(matrices.shape, jnp.bfloat16),
            vmem(pairs, 8, cols), vmem(pairs, 8, cols),
            vmem(2, members + 1, 2, 8, cols), vmem(2, 2, members + 1, 8, cols),
            vmem(pairs, 8, cols), vmem(pairs, 8, cols),
            vmem(2, members + 1, 2, 8, cols), vmem(2, 2, members + 1, 8, cols),
            vmem(members, layers + 1, SPAN, cols), vmem(fields, *tall), vmem(members, *tall),
            vmem(*tall), vmem(members, *tall),
            vmem(*each), vmem(*each), vmem(*each), vmem(*each), vmem(*each),
            vmem(2 + members, TALL, lanes),
            vmem(*core[1:]), vmem(*core), vmem(*core), vmem(*core), vmem(*core), vmem(*core[1:]),
            vmem(1, 1, cols), vmem(total, 1, cols), vmem(total - 1, 1, cols), vmem(2 * pairs + 8 * (members + 1), 8, cols),
            vmem(1 + 2 * members, *core[1:]),
            pltpu.SemaphoreType.REGULAR((rounds,)),
            pltpu.SemaphoreType.DMA((6,)),
            pltpu.SemaphoreType.DMA((members + 1,)), pltpu.SemaphoreType.DMA, pltpu.SemaphoreType.DMA,
        ],
        compiler_params=pltpu.CompilerParams(
            collective_id=0, has_side_effects=True, vmem_limit_bytes=40 << 20),
        name="picard",
    )(*[pltpu.with_memory_space_constraint(x, pltpu.HBM) for x in inputs])


def solution(mesh):
    sizes = (mesh.shape["plane"], mesh.shape["planey"], mesh.shape["ens"])
    in_specs = (
        P(("group", "ens"), None, None, "plane", "planey"),
        P(("group", "ens")),
        P("group", "plane", "planey"),
        P("plane", "planey"),
        P("plane", "planey"),
    )
    out_specs = P("group", None, "plane", "planey")
    return jax.shard_map(functools.partial(body, sizes), mesh=mesh, in_specs=in_specs,
                         out_specs=out_specs, check_vma=False)
```

```python
import functools
import math
import numpy as np
import jax
import jax.numpy as jnp
from jax import lax
from jax.experimental import pallas as pl
from jax.experimental.pallas import tpu as pltpu
from jax.sharding import PartitionSpec as P

bed_unit = 2.0 ** (-29)
HALO = 4
TOP = 8
SPAN = 24
TALL = 136
PAD = 160
STEP = 16
STEP_I = (0.25, 0.125)
STEP_J = (0.125, 0.25)


def iota(shape, dim):
    return lax.broadcasted_iota(jnp.int32, shape, dim)


def turn(x, step):
    return pltpu.roll(x, step % x.shape[1], 1)


def stencils(layers, lanes):
    def matrix(entry):
        out = np.zeros((lanes, lanes), np.float32)
        for z in range(layers):
            for i in range(-HALO, SPAN - HALO):
                for dz in (-1, 0, 1):
                    for di in (-1, 0, 1):
                        if 0 <= z + dz < layers and -HALO <= i + di < SPAN - HALO:
                            out[(z + dz) * SPAN + (i + di) % SPAN, z * SPAN + i % SPAN] = entry(dz, di)
        return out

    def copies(slot, targets, steps):
        out = np.zeros((lanes, lanes), np.float32)
        for z in targets:
            for i in range(-HALO, SPAN - HALO):
                for di, weight in steps:
                    if -HALO <= i + di < SPAN - HALO:
                        out[slot * SPAN + (i + di) % SPAN, z * SPAN + i % SPAN] = weight
        return out

    same, difference = ((0, 1.0),), ((1, 1.0), (-1, -1.0))
    every = range(layers)
    out = [matrix(lambda dz, di, c=c: (2.0 - abs(dz)) * (STEP_I[c] if di else 1.0)) for c in range(2)]
    out.append(matrix(lambda dz, di: 0.0 if dz else float(di)))
    out += [copies(1, every, same), copies(0, every, same), copies(0, every, difference)]
    return np.stack(out)


def kernel(sizes, rows_hbm, u_hbm, table_hbm, bed_hbm, mask_hbm, matrix_hbm, out_ref,
           rows_ref, flat, table_v, bed_v, mask_v, matrix,
           up_s, down_s, side_s, corner_s,
           below_r, above_r, side_r, corner_r,
           steep, tall, tall_steep, cover, roots, tr, pa, pb, r_ext, a_ext, force,
           w_core, r_core, a_core, r_peer, a_peer, w_peer, gram_s, gram_r, gram_blank, blank, wide_blank,
           relay, in_sem, halo_recv, peer_recv, gram_recv):
    np_, nq, ne = sizes
    other, layers, rows, cols = u_hbm.shape
    members = other // 2
    ix, iy, ie = lax.axis_index("plane"), lax.axis_index("planey"), lax.axis_index("ens")
    total = np_ * nq * ne
    mesh_id = pl.DeviceIdType.MESH
    fixed = 2 + members
    lanes = 2 * cols
    assert rows + 2 * HALO == SPAN and cols == 128 and layers * SPAN <= lanes
    assert fixed <= layers and fixed * SPAN <= cols
    halo_send, peer_send, gram_send = in_sem.at[0], in_sem.at[1], in_sem.at[2]

    reach = max(np_, nq)
    rounds = reach - 2 if reach > 3 else reach - 1

    def neighbours(every_core):
        found = []
        for dx, dy in ((-1, -1), (-1, 1), (1, -1), (1, 1), (-1, 0), (1, 0), (0, -1), (0, 1), (0, 0)):
            for de in range(ne):
                if (dx, dy, de) == (0, 0, 0) or (de and (dx or dy) and not every_core):
                    continue
                tx, ty = ix + dx, iy + dy
                ok = (tx >= 0) & (tx < np_) & (ty >= 0) & (ty < nq)
                where = {"plane": jnp.clip(tx, 0, np_ - 1), "planey": jnp.clip(ty, 0, nq - 1),
                         "ens": lax.rem(ie + de, ne)}
                found.append((ok if dx or dy else None, where))
        return found

    span_x = 1 + (ix > 0).astype(jnp.int32) + (ix < np_ - 1).astype(jnp.int32)
    span_y = 1 + (iy > 0).astype(jnp.int32) + (iy < nq - 1).astype(jnp.int32)
    near_count = span_x * span_y + ne - 2
    wide_count = span_x * span_y * ne - 1

    def signal(sem, every_core):
        for ok, where in neighbours(every_core):
            def tell(where=where):
                pl.semaphore_signal(sem, inc=1, device_id=where, device_id_type=mesh_id)
            tell() if ok is None else pl.when(ok)(tell)

    barrier = pltpu.get_barrier_semaphore()
    signal(barrier, False)

    loads = [
        pltpu.make_async_copy(src, dst, in_sem.at[i])
        for i, (src, dst) in enumerate(
            ((u_hbm, flat.at[pl.ds(0, other), pl.ds(0, layers), pl.ds(0, rows)]),
             (table_hbm, table_v), (bed_hbm, bed_v), (mask_hbm, mask_v), (rows_hbm, rows_ref),
             (matrix_hbm, matrix)))
    ]
    late = loads.pop()
    for load in loads:
        load.start()

    def group_place(d):
        de, rest = d // (np_ * nq), d % (np_ * nq)
        return (lax.rem(2 * np_ - 1 - ix + rest // nq, np_), lax.rem(2 * nq - 1 - iy + rest % nq, nq),
                lax.rem(ie + de, ne))

    def each_peer(fn):
        if total <= 32:
            for d in range(total):
                fn(d)
        else:
            def step(d, carry):
                fn(d)
                return carry
            lax.fori_loop(0, total, step, 0)

    planes = [[(other, k) for k in range(fixed + fixed % 2)]] + [
        [(2 * m + c, z) for z in range(layers) for c in range(2)] for m in range(members)]
    fields = [(other,)] + [(2 * m, 2 * m + 1) for m in range(members)]
    chunks = range(len(planes))
    pair_at = [sum(len(p) for p in planes[:k]) // 2 for k in chunks]
    pair_count = [len(p) // 2 for p in planes]

    has_up, has_down = ix > 0, ix < np_ - 1
    has_left, has_right = iy > 0, iy < nq - 1
    flows = [[] for _ in chunks]
    absent = []
    for dx, dy, src, dst in (
        (-1, -1, corner_s.at[0, 0], corner_r.at[1, 1]),
        (-1, 1, corner_s.at[0, 1], corner_r.at[1, 0]),
        (1, -1, corner_s.at[1, 0], corner_r.at[0, 1]),
        (1, 1, corner_s.at[1, 1], corner_r.at[0, 0]),
        (0, -1, side_s.at[0], side_r.at[1]),
        (0, 1, side_s.at[1], side_r.at[0]),
        (-1, 0, up_s, below_r),
        (1, 0, down_s, above_r),
    ):
        tx, ty = ix + dx, iy + dy
        sx, sy = ix - dx, iy - dy
        to_ok = (tx >= 0) & (tx < np_) & (ty >= 0) & (ty < nq)
        from_ok = (sx >= 0) & (sx < np_) & (sy >= 0) & (sy < nq)
        absent.append((jnp.logical_not(from_ok), dst))
        for k in chunks:
            part = pl.ds(k, 1) if dy else pl.ds(pair_at[k], pair_count[k])
            copy = pltpu.make_async_remote_copy(
                src_ref=src.at[part], dst_ref=dst.at[part],
                send_sem=halo_send, recv_sem=halo_recv.at[k],
                device_id={"plane": jnp.clip(tx, 0, np_ - 1), "planey": jnp.clip(ty, 0, nq - 1)},
                device_id_type=mesh_id)
            flows[k].append((to_ok, copy))

    def tiles(count):
        return blank.at[pl.ds(0, count)]

    def settle(chunk_list, received):
        for up in (0, 1):
            for down in (0, 1):
                for left in (0, 1):
                    for right in (0, 1):
                        if (up + down > np_ - 1 or left + right > nq - 1
                                or (np_ > 1 and up + down == 0) or (nq > 1 and left + right == 0)):
                            continue
                        count = sum(
                            pair_count[k] * (up + down) + (2 + up + down) * (left + right)
                            for k in chunk_list)
                        if count == 0:
                            continue
                        here = ((has_up == bool(up)) & (has_down == bool(down))
                                & (has_left == bool(left)) & (has_right == bool(right)))
                        bulk = pltpu.make_async_remote_copy(
                            src_ref=tiles(count), dst_ref=tiles(count), send_sem=halo_send,
                            recv_sem=halo_recv.at[chunk_list[0]],
                            device_id={"ens": lax.rem(ie + 1, ne)}, device_id_type=mesh_id)
                        pl.when(here)(bulk.wait_recv if received else bulk.wait_send)

    rim = jnp.zeros((SPAN - rows, cols), jnp.float32)
    for f in range(other + 1):
        flat[f, layers] = jnp.zeros((SPAN, cols), jnp.float32)
        for z in range(layers):
            flat[f, z, pl.ds(rows, SPAN - rows)] = rim
    for k in range(fixed, layers):
        flat[other, k, pl.ds(0, rows)] = jnp.zeros((rows, cols), jnp.float32)

    for load in loads:
        load.wait()
    late.start()

    cover_core = mask_v[...].astype(jnp.float32)
    flat[other, 0, pl.ds(0, rows)] = bed_v[...].astype(jnp.float32) * bed_unit
    flat[other, 1, pl.ds(0, rows)] = cover_core
    for m in range(members):
        flat[other, 2 + m, pl.ds(0, rows)] = table_v[rows_ref[m]]
    lane8 = iota((8, cols), 1)

    def places(start, offset):
        out = None
        for z in range(layers):
            low = z * SPAN + start - offset
            if -HALO < low < cols:
                here = (lane8 >= low) & (lane8 < low + HALO)
                out = here if out is None else out | here
        return out

    def stood_up(field):
        plain = field[...].reshape((layers + 1) * SPAN, cols)
        return [plain[cols * h:cols * (h + 1)].T for h in range(2)]

    def pack(k):
        for i, at in enumerate(planes[k]):
            half = pl.ds(HALO * (i % 2), HALO)
            up_s[pair_at[k] + i // 2, half] = flat[at + (pl.ds(0, HALO),)]
            down_s[pair_at[k] + i // 2, half] = flat[at + (pl.ds(rows - HALO, HALO),)]
        edges = []
        for f in fields[k]:
            halves = stood_up(flat.at[f])
            edges.append([[half[start:start + HALO] for half in halves] for start in (0, cols - HALO)])
        if len(edges) == 1:
            edges.append([[jnp.zeros((HALO, cols), jnp.float32)] * 2] * 2)
        for h in range(2):
            pair = [jnp.concatenate([edges[0][h][q], edges[1][h][q]], axis=0) for q in range(2)]
            side_s[h, k, 0] = pair[0]
            side_s[h, k, 1] = pair[1]
            corner_s[0, h, k] = jnp.where(places(0, 0), pair[0], pair[1])
            corner_s[1, h, k] = jnp.where(places(rows - HALO, 0), pair[0], pair[1])

    def send(k):
        for to_ok, copy in flows[k]:
            pl.when(to_ok)(copy.start)

    pack(0)
    pack(1)
    pl.semaphore_wait(barrier, near_count)
    send(0)
    send(1)
    for k in chunks[2:]:
        pack(k)
        send(k)
    if rounds > 0:
        signal(relay.at[0], False)

    for gone, dst in absent:
        @pl.when(gone)
        def _(dst=dst):
            dst[...] = jnp.zeros(dst.shape, jnp.float32)
    for c in range(2):
        for z in range(layers):
            summed = flat[c, z, pl.ds(0, rows)]
            for m in range(1, members):
                summed = summed + flat[2 * m + c, z, pl.ds(0, rows)]
            w_core[c, z] = cover_core * summed

    peer = {"ens": lax.rem(ie + 1, ne)}

    def to_peer(src, dst):
        return pltpu.make_async_remote_copy(
            src_ref=src, dst_ref=dst, send_sem=peer_send, recv_sem=peer_recv,
            device_id=peer, device_id_type=mesh_id)

    send_w = to_peer(w_core, w_peer)
    send_r = [to_peer(r_core.at[m], r_peer.at[m]) for m in range(members)]
    send_a = [to_peer(a_core.at[m], a_peer.at[m]) for m in range(members)]
    send_w.start()

    def relay_wait(k):
        pl.semaphore_wait(relay.at[k], wide_count if k else near_count)

    def relay_on(k):
        relay_wait(k - 1)
        signal(relay.at[k], True)

    if rounds > 1:
        relay_on(1)
    late.wait()

    def at(ref, index, base, count=TALL):
        return jnp.concatenate([ref[index + (q, pl.ds(base, count))] for q in range(2)], axis=1)

    def put(ref, index, base, value):
        for q in range(2):
            ref[index + (q, pl.ds(base, value.shape[0]))] = value[:, cols * q:cols * (q + 1)]

    def steepen(m, part):
        for z in range(layers):
            square = None
            for f in (2 * m, 2 * m + 1):
                change = None
                if z < layers - 1:
                    change = flat[f, z + 1, part]
                if z > 0:
                    change = flat[f, z - 1, part] if change is None else change - flat[f, z - 1, part]
                square = change * change if square is None else square + change * change
            steep[m, z, part] = square

    for m in range(members):
        steep[m, layers] = jnp.zeros((SPAN, cols), jnp.float32)
        steepen(m, pl.ds(0, rows))

    def assemble(k):
        for i, place in enumerate(planes[k]):
            half = pl.ds(HALO * (i % 2), HALO)
            pair = pair_at[k] + i // 2
            flat[place + (pl.ds(rows, HALO),)] = below_r[pair, half]
            flat[place + (pl.ds(rows + HALO, HALO),)] = above_r[pair, half]
        for h in range(2):
            over = turn(corner_r[0, h, k], SPAN - rows)
            under = turn(corner_r[1, h, k], rows)
            start = TOP + cols if h else TOP - HALO
            parts = []
            for q in range(2):
                part = jnp.where(places(rows + HALO, cols * q), over, side_r[h, k, q])
                part = jnp.where(places(rows, cols * q), under, part)
                for n, f in enumerate(fields[k]):
                    tall[f, q, pl.ds(start, HALO)] = part[HALO * n:HALO * (n + 1)]
                parts.append(part)
            if k:
                uppers, lowers = [turn(p, -SPAN) for p in parts], [turn(p, SPAN) for p in parts]
                for q in range(2):
                    whole = lane8 + cols * q
                    upper = jnp.where(lane8 < cols - SPAN, uppers[q], uppers[1 - q])
                    lower = jnp.where(lane8 >= SPAN, lowers[q], lowers[1 - q])
                    change = (jnp.where(whole < (layers - 1) * SPAN, upper, 0.0)
                              - jnp.where(whole >= SPAN, lower, 0.0))
                    change = change * change
                    tall_steep[k - 1, q, pl.ds(start, HALO)] = change[0:HALO] + change[HALO:2 * HALO]
        for f in fields[k]:
            for q, half in enumerate(stood_up(flat.at[f])):
                tall[f, q, pl.ds(TOP, cols)] = half
        if k:
            steepen(k - 1, pl.ds(rows, SPAN - rows))
            for q, half in enumerate(stood_up(steep.at[k - 1])):
                tall_steep[k - 1, q, pl.ds(TOP, cols)] = half

    def times(count, *jobs):
        steps_of = [(start, min(STEP, count - start)) for start in range(0, count, STEP)]
        parts = [[] for _ in jobs]
        for start, n in steps_of:
            for (_, makers), part in zip(jobs, parts):
                for maker in makers:
                    x = maker(start, n)
                    high = x.astype(jnp.bfloat16)
                    low = x - high.astype(jnp.float32)
                    if n == STEP:
                        part += [high, low.astype(jnp.bfloat16)]
                    else:
                        part.append(jnp.concatenate([x, low], axis=0).astype(jnp.bfloat16))
        outs = [jnp.dot(jnp.concatenate(part, axis=0), matrix[k], preferred_element_type=jnp.float32)
                for (k, _), part in zip(jobs, parts)]

        def piece(out, low, n):
            return out[low:low + n] + out[low + n:low + 2 * n]

        return [(start, n, [[piece(out, 2 * (start * len(makers) + n * i), n) for i in range(len(makers))]
                            for (_, makers), out in zip(jobs, outs)]) for start, n in steps_of]

    root_base, res_base, img_base = TOP - 3, TOP - 2, TOP - 1
    lane = iota((8, lanes), 1)
    layer = sum([(lane >= SPAN * z).astype(jnp.int32) for z in range(1, layers + 1)])
    place = lane - SPAN * layer
    inside = ((place < rows) & (layer < layers)).astype(jnp.float32)[0:1]

    def prepare():
        put(cover, (), root_base, jnp.dot(
            at(tall, (other,), root_base, TALL + 8).astype(jnp.bfloat16), matrix[3],
            preferred_element_type=jnp.float32))

    def prepare_force():
        b = res_base
        row = (ix * rows + jnp.where(place < rows + HALO, place, place - SPAN))[0:1]
        thickness = 1.0 + 2.0 * row.astype(jnp.float32) / (np_ * rows - 1)

        ground = iota((STEP, cols), 1) < SPAN

        def field(start, n):
            return at(tall, (other,), b + start, n)

        def across(start, n):
            return at(tall, (other,), b + start + 1, n) - at(tall, (other,), b + start - 1, n)

        products = times(TALL, (5, [field]), (4, [across]))
        yield
        for start, n, ((slope_x,), (slope_y,)) in products:
            covered = at(cover, (), b + start, n)
            here = pl.ds(start, n)
            force[0, here] = -(covered * thickness * (slope_x * 0.5))
            force[1, here] = -(covered * thickness * (slope_y * 0.5))
            dry = 1.0 - covered
            for m in range(members):
                rub = turn(tall[other, 0, pl.ds(b + start, n)], -SPAN * (2 + m))
                rub = jnp.where(ground[0:n], covered[:, 0:cols] * rub, 0.0)
                force[2 + m, here] = jnp.concatenate([dry[:, 0:cols] + rub, dry[:, cols:]], axis=1)
            yield

    def roots_level(m):
        b = root_base

        def u(start, n, shift=0):
            return at(tall, (2 * m,), b + start + shift, n)

        def v(start, n, shift=0):
            return at(tall, (2 * m + 1,), b + start + shift, n)

        products = times(TALL, (2, [u, v]))
        yield
        for start, n, ((u_i, v_i),) in products:
            u_j, v_j = u(start, n, 1) - u(start, n, -1), v(start, n, 1) - v(start, n, -1)
            shear = u_j + v_i
            strain = (4.0 * (u_i * (u_i + v_j) + v_j * v_j) + shear * shear
                      + (at(tall_steep, (m,), b + start, n) + 1.6))
            root = at(cover, (), b + start, n) * jnp.exp2(
                jnp.log(strain) * (-1.0 / (6.0 * math.log(2.0))) + (0.5 + 4.0 / 6.0))
            put(roots, (m,), b + start, root)
            put(pa, (m, 0), b + start, root * u(start, n))
            put(pa, (m, 1), b + start, root * v(start, n))
            yield

    def leaning(ref, index, base, steps, known=None):
        def maker(start, n):
            low = base + start
            found = None if known is None else known.pop(start, None)
            if found is None:
                found = at(ref, index, low, n), at(ref, index, low - 1, n) + at(ref, index, low + 1, n)
                if known is not None:
                    known[start] = found
            return found[0] + steps * found[1]
        return maker

    def residual_level(m):
        b, known = res_base, {}
        products = times(TALL, *[
            (c, [leaning(roots, (m,), b, STEP_J[c], known), leaning(pa, (m, c), b, STEP_J[c])])
            for c in range(2)])
        yield
        for start, n, pairs in products:
            for c, (near, moved) in enumerate(pairs):
                low, here = b + start, pl.ds(start, n)
                root = at(roots, (m,), low, n)
                weight = root * near + force[2 + m, here]
                r = force[c, here] - (weight * (at(cover, (), low, n) * at(tall, (2 * m + c,), low, n))
                                      - root * moved)
                put(tr, (m, c), low, weight)
                put(r_ext, (m, c), low, r)
                put(pb, (m, c), low, root * r)
            yield

    def image_level(m):
        b = img_base
        products = times(TALL, *[(c, [leaning(pb, (m, c), b, STEP_J[c])]) for c in range(2)])
        yield
        for start, n, pairs in products:
            for c, (moved,) in enumerate(pairs):
                low = b + start
                root = at(roots, (m,), low, n)
                a = at(tr, (m, c), low, n) * at(r_ext, (m, c), low, n) - root * moved
                put(a_ext, (m, c), low, a)
                put(pa, (m, c), low, root * a)
            yield

    grams = [None] * members

    def second_level(m):
        def one_way(c):
            def maker(start, n):
                low = TOP + start
                return at(pa, (m, c), low, n) + (2.0 * STEP_J[c]) * at(pa, (m, c), low - 1, n)
            return maker

        products = times(cols, *[(c, [one_way(c)]) for c in range(2)])
        yield
        sums = None
        for start, n, pairs in products:
            for c, (out,) in enumerate(pairs):
                low = TOP + start
                r, a = at(r_ext, (m, c), low, n), at(a_ext, (m, c), low, n)
                square = a * a
                terms = (r * r, r * a, square,
                         at(tr, (m, c), low, n) * square - at(pa, (m, c), low, n) * out)
                sums = terms if sums is None else [s + t for s, t in zip(sums, terms)]
            yield
        grams[m] = [inside * jnp.sum(s, axis=0, keepdims=True) for s in sums]

    def together(*levels):
        levels = list(levels)
        while levels:
            for level in list(levels):
                try:
                    next(level)
                except StopIteration:
                    levels.remove(level)

    settle([0], True)
    settle([1], True)
    assemble(0)
    assemble(1)
    prepare()
    together(roots_level(0), prepare_force())
    for k in range(2, rounds):
        relay_on(k)
    stages = (roots_level, residual_level, image_level, second_level)
    for turn_of in range(1, members + len(stages) - 1):
        if turn_of < members:
            settle([1 + turn_of], True)
            assemble(1 + turn_of)
        together(*[stages[turn_of - m](m) for m in range(members) if 0 <= turn_of - m < len(stages)])

    lane_1 = iota((1, cols), 1)
    mine = jnp.zeros((1, cols), jnp.float32)
    for m in range(members):
        for q, acc in enumerate(grams[m]):
            mine = jnp.where(lane_1 == 4 * m + q, jnp.sum(acc, axis=1, keepdims=True), mine)
    gram_s[0] = mine

    if rounds > 0:
        relay_wait(rounds - 1)

    def send_gram(d):
        px, py, pe = group_place(d)
        copy = pltpu.make_async_remote_copy(
            src_ref=gram_s, dst_ref=gram_r.at[pl.ds(d, 1)],
            send_sem=gram_send, recv_sem=gram_recv,
            device_id={"plane": px, "planey": py, "ens": pe}, device_id_type=mesh_id)
        own = (px == ix) & (py == iy) & (pe == ie)
        pl.when(jnp.logical_not(own))(copy.start)

    each_peer(send_gram)
    own_place = lax.rem(2 * ix + 1, np_) * nq + lax.rem(2 * iy + 1, nq)
    gram_r[pl.ds(own_place, 1)] = mine[None]

    def lie_down(src, dst):
        for c in range(2):
            flat_rows = jnp.concatenate(
                [src[c, q, pl.ds(TOP, cols)].T for q in range(2)], axis=0)
            for z in range(layers):
                dst[c, z] = flat_rows[SPAN * z:SPAN * z + rows]

    for m in range(members):
        lie_down(r_ext.at[m], r_core.at[m])
        send_r[m].start()
        lie_down(a_ext.at[m], a_core.at[m])
        send_a[m].start()
    everything = pltpu.make_async_remote_copy(
        src_ref=gram_blank, dst_ref=gram_blank, send_sem=gram_send, recv_sem=gram_recv,
        device_id=peer, device_id_type=mesh_id)
    everything.wait_recv()

    half = np_ * nq
    sums = [jnp.sum(gram_r[half * e:half * (e + 1)], axis=0) for e in range(ne)]
    steps = []
    for e in range(ne):
        for m in range(members):
            g_rr, g_ra, g_aa, g_ab = [
                jnp.sum(jnp.where(lane_1 == 4 * m + q, sums[e], 0.0), axis=1, keepdims=True)
                for q in range(4)
            ]
            first_step = g_rr / g_ra
            following = g_rr - 2.0 * first_step * g_ra + first_step * first_step * g_aa
            growth = 1.0 + following / g_rr
            curve = (growth * growth * g_ra - 2.0 * growth * first_step * g_aa
                     + first_step * first_step * g_ab)
            second_step = following / curve
            share = 1.0 / (members * ne)
            steps.append(((first_step + second_step * growth) * share,
                          second_step * first_step * share))

    peer_part = wide_blank.at[pl.ds(0, 1 + 2 * members)]
    peer_bulk = to_peer(peer_part, peer_part)
    peer_bulk.wait_recv()
    share = 1.0 / (members * ne)

    def final_step(z):
        for c in range(2):
            value = share * (w_core[c, z] + w_peer[c, z])
            for m in range(members):
                one, two = steps[m]
                value = value + one * r_core[m, c, z] - two * a_core[m, c, z]
                one, two = steps[members + m]
                value = value + one * r_peer[m, c, z] - two * a_peer[m, c, z]
            out_ref[c, z] = value

    for z in range(layers):
        final_step(z)

    settle(list(chunks), False)
    peer_bulk.wait_send()
    everything.wait_send()


def body(sizes, u_prior, friction_rows, friction_table, bed_fixed, ice_mask):
    members, _, layers, rows, cols = u_prior.shape
    levels = friction_table.shape[0]
    total = sizes[0] * sizes[1] * sizes[2]
    fixed = 2 + members
    pairs = (fixed + fixed % 2 + members * 2 * layers) // 2
    fields, lanes = 2 * members + 1, 2 * cols
    rounds = max(max(sizes[0], sizes[1]) - 2, 2)
    f32 = jnp.float32
    matrices = jnp.asarray(stencils(layers, lanes), jnp.bfloat16)
    any_space = pl.BlockSpec(memory_space=pl.ANY)
    vmem = lambda *shape: pltpu.VMEM(shape, f32)
    core = (members, 2, layers, rows, cols)
    tall = (2, PAD, cols)
    each = (members, 2) + tall
    inputs = (friction_rows, u_prior.reshape((-1,) + u_prior.shape[2:]), friction_table, bed_fixed, ice_mask, matrices)
    return pl.pallas_call(
        functools.partial(kernel, sizes),
        out_shape=pltpu.VMEM((2, layers, rows, cols), f32),
        in_specs=[any_space] * 6,
        out_specs=pl.BlockSpec(memory_space=pltpu.VMEM),
        scratch_shapes=[
            pltpu.SMEM((members,), jnp.int32), vmem(fields, layers + 1, SPAN, cols),
            vmem(levels, rows, cols),
            pltpu.VMEM((rows, cols), jnp.int32), pltpu.VMEM((rows, cols), jnp.int32),
            pltpu.VMEM(matrices.shape, jnp.bfloat16),
            vmem(pairs, 8, cols), vmem(pairs, 8, cols),
            vmem(2, members + 1, 2, 8, cols), vmem(2, 2, members + 1, 8, cols),
            vmem(pairs, 8, cols), vmem(pairs, 8, cols),
            vmem(2, members + 1, 2, 8, cols), vmem(2, 2, members + 1, 8, cols),
            vmem(members, layers + 1, SPAN, cols), vmem(fields, *tall), vmem(members, *tall),
            vmem(*tall), vmem(members, *tall),
            vmem(*each), vmem(*each), vmem(*each), vmem(*each), vmem(*each),
            vmem(2 + members, TALL, lanes),
            vmem(*core[1:]), vmem(*core), vmem(*core), vmem(*core), vmem(*core), vmem(*core[1:]),
            vmem(1, 1, cols), vmem(total, 1, cols), vmem(total - 1, 1, cols), vmem(2 * pairs + 8 * (members + 1), 8, cols),
            vmem(1 + 2 * members, *core[1:]),
            pltpu.SemaphoreType.REGULAR((rounds,)),
            pltpu.SemaphoreType.DMA((6,)),
            pltpu.SemaphoreType.DMA((members + 1,)), pltpu.SemaphoreType.DMA, pltpu.SemaphoreType.DMA,
        ],
        compiler_params=pltpu.CompilerParams(
            collective_id=0, has_side_effects=True, vmem_limit_bytes=40 << 20),
        name="picard",
    )(*[pltpu.with_memory_space_constraint(x, pltpu.HBM) for x in inputs])


def solution(mesh):
    sizes = (mesh.shape["plane"], mesh.shape["planey"], mesh.shape["ens"])
    in_specs = (
        P(("group", "ens"), None, None, "plane", "planey"),
        P(("group", "ens")),
        P("group", "plane", "planey"),
        P("plane", "planey"),
        P("plane", "planey"),
    )
    out_specs = P("group", None, "plane", "planey")
    return jax.shard_map(functools.partial(body, sizes), mesh=mesh, in_specs=in_specs,
                         out_specs=out_specs, check_vma=False)
```

```python
import functools
import math
import numpy as np
import jax
import jax.numpy as jnp
from jax import lax
from jax.experimental import pallas as pl
from jax.experimental.pallas import tpu as pltpu
from jax.sharding import PartitionSpec as P

bed_unit = 2.0 ** (-29)
HALO = 4
TOP = 8
SPAN = 24
TALL = 136
PAD = 160
STEP = 16
STEP_I = (0.25, 0.125)
STEP_J = (0.125, 0.25)


def iota(shape, dim):
    return lax.broadcasted_iota(jnp.int32, shape, dim)


def turn(x, step):
    return pltpu.roll(x, step % x.shape[1], 1)


def stencils(layers, lanes):
    def matrix(entry):
        out = np.zeros((lanes, lanes), np.float32)
        for z in range(layers):
            for i in range(-HALO, SPAN - HALO):
                for dz in (-1, 0, 1):
                    for di in (-1, 0, 1):
                        if 0 <= z + dz < layers and -HALO <= i + di < SPAN - HALO:
                            out[(z + dz) * SPAN + (i + di) % SPAN, z * SPAN + i % SPAN] = entry(dz, di)
        return out

    def copies(slot, targets, steps):
        out = np.zeros((lanes, lanes), np.float32)
        for z in targets:
            for i in range(-HALO, SPAN - HALO):
                for di, weight in steps:
                    if -HALO <= i + di < SPAN - HALO:
                        out[slot * SPAN + (i + di) % SPAN, z * SPAN + i % SPAN] = weight
        return out

    same, difference = ((0, 1.0),), ((1, 1.0), (-1, -1.0))
    every = range(layers)
    out = [matrix(lambda dz, di, c=c: (2.0 - abs(dz)) * (STEP_I[c] if di else 1.0)) for c in range(2)]
    out.append(matrix(lambda dz, di: 0.0 if dz else float(di)))
    out += [copies(1, every, same), copies(0, every, same), copies(0, every, difference)]
    return np.stack(out)


def kernel(sizes, rows_hbm, u_hbm, table_hbm, bed_hbm, mask_hbm, matrix_hbm, out_ref,
           rows_ref, flat, table_v, bed_v, mask_v, matrix,
           up_s, down_s, side_s, corner_s,
           below_r, above_r, side_r, corner_r,
           steep, tall, tall_steep, cover, roots, tr, pa, pb, r_ext, a_ext, force,
           w_core, r_core, a_core, r_peer, a_peer, w_peer, gram_s, gram_r, gram_blank, blank, wide_blank,
           relay, in_sem, halo_recv, peer_recv, gram_recv):
    np_, nq, ne = sizes
    other, layers, rows, cols = u_hbm.shape
    members = other // 2
    ix, iy, ie = lax.axis_index("plane"), lax.axis_index("planey"), lax.axis_index("ens")
    total = np_ * nq * ne
    mesh_id = pl.DeviceIdType.MESH
    fixed = 2 + members
    lanes = 2 * cols
    assert rows + 2 * HALO == SPAN and cols == 128 and layers * SPAN <= lanes
    assert fixed <= layers and fixed * SPAN <= cols
    halo_send, peer_send, gram_send = in_sem.at[0], in_sem.at[1], in_sem.at[2]

    reach = max(np_, nq)
    rounds = reach - 2 if reach > 3 else reach - 1

    def neighbours(every_core):
        found = []
        for dx, dy in ((-1, -1), (-1, 1), (1, -1), (1, 1), (-1, 0), (1, 0), (0, -1), (0, 1), (0, 0)):
            for de in range(ne):
                if (dx, dy, de) == (0, 0, 0) or (de and (dx or dy) and not every_core):
                    continue
                tx, ty = ix + dx, iy + dy
                ok = (tx >= 0) & (tx < np_) & (ty >= 0) & (ty < nq)
                where = {"plane": jnp.clip(tx, 0, np_ - 1), "planey": jnp.clip(ty, 0, nq - 1),
                         "ens": lax.rem(ie + de, ne)}
                found.append((ok if dx or dy else None, where))
        return found

    span_x = 1 + (ix > 0).astype(jnp.int32) + (ix < np_ - 1).astype(jnp.int32)
    span_y = 1 + (iy > 0).astype(jnp.int32) + (iy < nq - 1).astype(jnp.int32)
    near_count = span_x * span_y + ne - 2
    wide_count = span_x * span_y * ne - 1

    def signal(sem, every_core):
        for ok, where in neighbours(every_core):
            def tell(where=where):
                pl.semaphore_signal(sem, inc=1, device_id=where, device_id_type=mesh_id)
            tell() if ok is None else pl.when(ok)(tell)

    barrier = pltpu.get_barrier_semaphore()
    signal(barrier, False)

    loads = [
        pltpu.make_async_copy(src, dst, in_sem.at[i])
        for i, (src, dst) in enumerate(
            ((u_hbm, flat.at[pl.ds(0, other), pl.ds(0, layers), pl.ds(0, rows)]),
             (table_hbm, table_v), (bed_hbm, bed_v), (mask_hbm, mask_v), (rows_hbm, rows_ref),
             (matrix_hbm, matrix)))
    ]
    late = loads.pop()
    for load in loads:
        load.start()

    def group_place(d):
        de, rest = d // (np_ * nq), d % (np_ * nq)
        return (lax.rem(2 * np_ - 1 - ix + rest // nq, np_), lax.rem(2 * nq - 1 - iy + rest % nq, nq),
                lax.rem(ie + de, ne))

    def each_peer(fn):
        if total <= 32:
            for d in range(total):
                fn(d)
        else:
            def step(d, carry):
                fn(d)
                return carry
            lax.fori_loop(0, total, step, 0)

    planes = [[(other, k) for k in range(fixed + fixed % 2)]] + [
        [(2 * m + c, z) for z in range(layers) for c in range(2)] for m in range(members)]
    fields = [(other,)] + [(2 * m, 2 * m + 1) for m in range(members)]
    chunks = range(len(planes))
    pair_at = [sum(len(p) for p in planes[:k]) // 2 for k in chunks]
    pair_count = [len(p) // 2 for p in planes]

    has_up, has_down = ix > 0, ix < np_ - 1
    has_left, has_right = iy > 0, iy < nq - 1
    flows = [[] for _ in chunks]
    absent = []
    for dx, dy, src, dst in (
        (-1, -1, corner_s.at[0, 0], corner_r.at[1, 1]),
        (-1, 1, corner_s.at[0, 1], corner_r.at[1, 0]),
        (1, -1, corner_s.at[1, 0], corner_r.at[0, 1]),
        (1, 1, corner_s.at[1, 1], corner_r.at[0, 0]),
        (0, -1, side_s.at[0], side_r.at[1]),
        (0, 1, side_s.at[1], side_r.at[0]),
        (-1, 0, up_s, below_r),
        (1, 0, down_s, above_r),
    ):
        tx, ty = ix + dx, iy + dy
        sx, sy = ix - dx, iy - dy
        to_ok = (tx >= 0) & (tx < np_) & (ty >= 0) & (ty < nq)
        from_ok = (sx >= 0) & (sx < np_) & (sy >= 0) & (sy < nq)
        absent.append((jnp.logical_not(from_ok), dst))
        for k in chunks:
            part = pl.ds(k, 1) if dy else pl.ds(pair_at[k], pair_count[k])
            copy = pltpu.make_async_remote_copy(
                src_ref=src.at[part], dst_ref=dst.at[part],
                send_sem=halo_send, recv_sem=halo_recv.at[k],
                device_id={"plane": jnp.clip(tx, 0, np_ - 1), "planey": jnp.clip(ty, 0, nq - 1)},
                device_id_type=mesh_id)
            flows[k].append((to_ok, copy))

    def tiles(count):
        return blank.at[pl.ds(0, count)]

    def settle(chunk_list, received):
        for up in (0, 1):
            for down in (0, 1):
                for left in (0, 1):
                    for right in (0, 1):
                        if (up + down > np_ - 1 or left + right > nq - 1
                                or (np_ > 1 and up + down == 0) or (nq > 1 and left + right == 0)):
                            continue
                        count = sum(
                            pair_count[k] * (up + down) + (2 + up + down) * (left + right)
                            for k in chunk_list)
                        if count == 0:
                            continue
                        here = ((has_up == bool(up)) & (has_down == bool(down))
                                & (has_left == bool(left)) & (has_right == bool(right)))
                        bulk = pltpu.make_async_remote_copy(
                            src_ref=tiles(count), dst_ref=tiles(count), send_sem=halo_send,
                            recv_sem=halo_recv.at[chunk_list[0]],
                            device_id={"ens": lax.rem(ie + 1, ne)}, device_id_type=mesh_id)
                        pl.when(here)(bulk.wait_recv if received else bulk.wait_send)

    rim = jnp.zeros((SPAN - rows, cols), jnp.float32)
    for f in range(other + 1):
        flat[f, layers] = jnp.zeros((SPAN, cols), jnp.float32)
        for z in range(layers):
            flat[f, z, pl.ds(rows, SPAN - rows)] = rim
    for k in range(fixed, layers):
        flat[other, k, pl.ds(0, rows)] = jnp.zeros((rows, cols), jnp.float32)

    for load in loads:
        load.wait()
    late.start()

    cover_core = mask_v[...].astype(jnp.float32)
    flat[other, 0, pl.ds(0, rows)] = bed_v[...].astype(jnp.float32) * bed_unit
    flat[other, 1, pl.ds(0, rows)] = cover_core
    for m in range(members):
        flat[other, 2 + m, pl.ds(0, rows)] = table_v[rows_ref[m]]
    lane8 = iota((8, cols), 1)

    def places(start, offset):
        out = None
        for z in range(layers):
            low = z * SPAN + start - offset
            if -HALO < low < cols:
                here = (lane8 >= low) & (lane8 < low + HALO)
                out = here if out is None else out | here
        return out

    def stood_up(field):
        plain = field[...].reshape((layers + 1) * SPAN, cols)
        return [plain[cols * h:cols * (h + 1)].T for h in range(2)]

    def pack(k):
        for i, at in enumerate(planes[k]):
            half = pl.ds(HALO * (i % 2), HALO)
            up_s[pair_at[k] + i // 2, half] = flat[at + (pl.ds(0, HALO),)]
            down_s[pair_at[k] + i // 2, half] = flat[at + (pl.ds(rows - HALO, HALO),)]
        edges = []
        for f in fields[k]:
            halves = stood_up(flat.at[f])
            edges.append([[half[start:start + HALO] for half in halves] for start in (0, cols - HALO)])
        if len(edges) == 1:
            edges.append([[jnp.zeros((HALO, cols), jnp.float32)] * 2] * 2)
        for h in range(2):
            pair = [jnp.concatenate([edges[0][h][q], edges[1][h][q]], axis=0) for q in range(2)]
            side_s[h, k, 0] = pair[0]
            side_s[h, k, 1] = pair[1]
            corner_s[0, h, k] = jnp.where(places(0, 0), pair[0], pair[1])
            corner_s[1, h, k] = jnp.where(places(rows - HALO, 0), pair[0], pair[1])

    def send(k):
        for to_ok, copy in flows[k]:
            pl.when(to_ok)(copy.start)

    pack(0)
    pack(1)
    pl.semaphore_wait(barrier, near_count)
    send(0)
    send(1)
    for k in chunks[2:]:
        pack(k)
        send(k)
    if rounds > 0:
        signal(relay.at[0], False)

    for gone, dst in absent:
        @pl.when(gone)
        def _(dst=dst):
            dst[...] = jnp.zeros(dst.shape, jnp.float32)
    for c in range(2):
        for z in range(layers):
            summed = flat[c, z, pl.ds(0, rows)]
            for m in range(1, members):
                summed = summed + flat[2 * m + c, z, pl.ds(0, rows)]
            w_core[c, z] = cover_core * summed

    peer = {"ens": lax.rem(ie + 1, ne)}

    def to_peer(src, dst):
        return pltpu.make_async_remote_copy(
            src_ref=src, dst_ref=dst, send_sem=peer_send, recv_sem=peer_recv,
            device_id=peer, device_id_type=mesh_id)

    send_w = to_peer(w_core, w_peer)
    send_r = [to_peer(r_core.at[m], r_peer.at[m]) for m in range(members)]
    send_a = [to_peer(a_core.at[m], a_peer.at[m]) for m in range(members)]
    send_w.start()

    def relay_wait(k):
        pl.semaphore_wait(relay.at[k], wide_count if k else near_count)

    def relay_on(k):
        relay_wait(k - 1)
        signal(relay.at[k], True)

    if rounds > 1:
        relay_on(1)
    late.wait()

    def at(ref, index, base, count=TALL):
        return jnp.concatenate([ref[index + (q, pl.ds(base, count))] for q in range(2)], axis=1)

    def put(ref, index, base, value):
        for q in range(2):
            ref[index + (q, pl.ds(base, value.shape[0]))] = value[:, cols * q:cols * (q + 1)]

    def steepen(m, part):
        for z in range(layers):
            square = None
            for f in (2 * m, 2 * m + 1):
                change = None
                if z < layers - 1:
                    change = flat[f, z + 1, part]
                if z > 0:
                    change = flat[f, z - 1, part] if change is None else change - flat[f, z - 1, part]
                square = change * change if square is None else square + change * change
            steep[m, z, part] = square

    for m in range(members):
        steep[m, layers] = jnp.zeros((SPAN, cols), jnp.float32)
        steepen(m, pl.ds(0, rows))

    def assemble(k):
        for i, place in enumerate(planes[k]):
            half = pl.ds(HALO * (i % 2), HALO)
            pair = pair_at[k] + i // 2
            flat[place + (pl.ds(rows, HALO),)] = below_r[pair, half]
            flat[place + (pl.ds(rows + HALO, HALO),)] = above_r[pair, half]
        for h in range(2):
            over = turn(corner_r[0, h, k], SPAN - rows)
            under = turn(corner_r[1, h, k], rows)
            start = TOP + cols if h else TOP - HALO
            parts = []
            for q in range(2):
                part = jnp.where(places(rows + HALO, cols * q), over, side_r[h, k, q])
                part = jnp.where(places(rows, cols * q), under, part)
                for n, f in enumerate(fields[k]):
                    tall[f, q, pl.ds(start, HALO)] = part[HALO * n:HALO * (n + 1)]
                parts.append(part)
            if k:
                uppers, lowers = [turn(p, -SPAN) for p in parts], [turn(p, SPAN) for p in parts]
                for q in range(2):
                    whole = lane8 + cols * q
                    upper = jnp.where(lane8 < cols - SPAN, uppers[q], uppers[1 - q])
                    lower = jnp.where(lane8 >= SPAN, lowers[q], lowers[1 - q])
                    change = (jnp.where(whole < (layers - 1) * SPAN, upper, 0.0)
                              - jnp.where(whole >= SPAN, lower, 0.0))
                    change = change * change
                    tall_steep[k - 1, q, pl.ds(start, HALO)] = change[0:HALO] + change[HALO:2 * HALO]
        for f in fields[k]:
            for q, half in enumerate(stood_up(flat.at[f])):
                tall[f, q, pl.ds(TOP, cols)] = half
        if k:
            steepen(k - 1, pl.ds(rows, SPAN - rows))
            for q, half in enumerate(stood_up(steep.at[k - 1])):
                tall_steep[k - 1, q, pl.ds(TOP, cols)] = half

    def times(count, *jobs):
        steps_of = [(start, min(STEP, count - start)) for start in range(0, count, STEP)]
        parts = [[] for _ in jobs]
        for start, n in steps_of:
            for (_, makers), part in zip(jobs, parts):
                for maker in makers:
                    x = maker(start, n)
                    high = x.astype(jnp.bfloat16)
                    low = x - high.astype(jnp.float32)
                    if n == STEP:
                        part += [high, low.astype(jnp.bfloat16)]
                    else:
                        part.append(jnp.concatenate([x, low], axis=0).astype(jnp.bfloat16))
        outs = [jnp.dot(jnp.concatenate(part, axis=0), matrix[k], preferred_element_type=jnp.float32)
                for (k, _), part in zip(jobs, parts)]

        def piece(out, low, n):
            return out[low:low + n] + out[low + n:low + 2 * n]

        return [(start, n, [[piece(out, 2 * (start * len(makers) + n * i), n) for i in range(len(makers))]
                            for (_, makers), out in zip(jobs, outs)]) for start, n in steps_of]

    root_base, res_base, img_base = TOP - 3, TOP - 2, TOP - 1
    lane = iota((8, lanes), 1)
    layer = sum([(lane >= SPAN * z).astype(jnp.int32) for z in range(1, layers + 1)])
    place = lane - SPAN * layer
    inside = ((place < rows) & (layer < layers)).astype(jnp.float32)[0:1]

    def prepare():
        put(cover, (), root_base, jnp.dot(
            at(tall, (other,), root_base, TALL + 8).astype(jnp.bfloat16), matrix[3],
            preferred_element_type=jnp.float32))

    def prepare_force():
        b = res_base
        row = (ix * rows + jnp.where(place < rows + HALO, place, place - SPAN))[0:1]
        thickness = 1.0 + 2.0 * row.astype(jnp.float32) / (np_ * rows - 1)

        ground = iota((STEP, cols), 1) < SPAN

        def field(start, n):
            return at(tall, (other,), b + start, n)

        def across(start, n):
            return at(tall, (other,), b + start + 1, n) - at(tall, (other,), b + start - 1, n)

        products = times(TALL, (5, [field]), (4, [across]))
        yield
        for start, n, ((slope_x,), (slope_y,)) in products:
            covered = at(cover, (), b + start, n)
            here = pl.ds(start, n)
            force[0, here] = -(covered * thickness * (slope_x * 0.5))
            force[1, here] = -(covered * thickness * (slope_y * 0.5))
            dry = 1.0 - covered
            for m in range(members):
                rub = turn(tall[other, 0, pl.ds(b + start, n)], -SPAN * (2 + m))
                rub = jnp.where(ground[0:n], covered[:, 0:cols] * rub, 0.0)
                force[2 + m, here] = jnp.concatenate([dry[:, 0:cols] + rub, dry[:, cols:]], axis=1)
            yield

    def roots_level(m):
        b = root_base

        def u(start, n, shift=0):
            return at(tall, (2 * m,), b + start + shift, n)

        def v(start, n, shift=0):
            return at(tall, (2 * m + 1,), b + start + shift, n)

        products = times(TALL, (2, [u, v]))
        yield
        for start, n, ((u_i, v_i),) in products:
            u_j, v_j = u(start, n, 1) - u(start, n, -1), v(start, n, 1) - v(start, n, -1)
            shear = u_j + v_i
            strain = (4.0 * (u_i * (u_i + v_j) + v_j * v_j) + shear * shear
                      + (at(tall_steep, (m,), b + start, n) + 1.6))
            root = at(cover, (), b + start, n) * jnp.exp2(
                jnp.log(strain) * (-1.0 / (6.0 * math.log(2.0))) + (0.5 + 4.0 / 6.0))
            put(roots, (m,), b + start, root)
            put(pa, (m, 0), b + start, root * u(start, n))
            put(pa, (m, 1), b + start, root * v(start, n))
            yield

    def leaning(ref, index, base, steps, known=None):
        def maker(start, n):
            low = base + start
            found = None if known is None else known.pop(start, None)
            if found is None:
                found = at(ref, index, low, n), at(ref, index, low - 1, n) + at(ref, index, low + 1, n)
                if known is not None:
                    known[start] = found
            return found[0] + steps * found[1]
        return maker

    def residual_level(m):
        b, known = res_base, {}
        products = times(TALL, *[
            (c, [leaning(roots, (m,), b, STEP_J[c], known), leaning(pa, (m, c), b, STEP_J[c])])
            for c in range(2)])
        yield
        for start, n, pairs in products:
            for c, (near, moved) in enumerate(pairs):
                low, here = b + start, pl.ds(start, n)
                root = at(roots, (m,), low, n)
                weight = root * near + force[2 + m, here]
                r = force[c, here] - (weight * (at(cover, (), low, n) * at(tall, (2 * m + c,), low, n))
                                      - root * moved)
                put(tr, (m, c), low, weight)
                put(r_ext, (m, c), low, r)
                put(pb, (m, c), low, root * r)
            yield

    def image_level(m):
        b = img_base
        products = times(TALL, *[(c, [leaning(pb, (m, c), b, STEP_J[c])]) for c in range(2)])
        yield
        for start, n, pairs in products:
            for c, (moved,) in enumerate(pairs):
                low = b + start
                root = at(roots, (m,), low, n)
                a = at(tr, (m, c), low, n) * at(r_ext, (m, c), low, n) - root * moved
                put(a_ext, (m, c), low, a)
                put(pa, (m, c), low, root * a)
            yield

    grams = [None] * members

    def second_level(m):
        def one_way(c):
            def maker(start, n):
                low = TOP + start
                return at(pa, (m, c), low, n) + (2.0 * STEP_J[c]) * at(pa, (m, c), low - 1, n)
            return maker

        products = times(cols, *[(c, [one_way(c)]) for c in range(2)])
        yield
        sums = None
        for start, n, pairs in products:
            for c, (out,) in enumerate(pairs):
                low = TOP + start
                r, a = at(r_ext, (m, c), low, n), at(a_ext, (m, c), low, n)
                square = a * a
                terms = (r * r, r * a, square,
                         at(tr, (m, c), low, n) * square - at(pa, (m, c), low, n) * out)
                sums = terms if sums is None else [s + t for s, t in zip(sums, terms)]
            yield
        grams[m] = [inside * jnp.sum(s, axis=0, keepdims=True) for s in sums]

    def together(*levels):
        levels = list(levels)
        while levels:
            for level in list(levels):
                try:
                    next(level)
                except StopIteration:
                    levels.remove(level)

    settle([0], True)
    settle([1], True)
    assemble(0)
    assemble(1)
    prepare()
    together(roots_level(0), prepare_force())
    for k in range(2, rounds):
        relay_on(k)
    stages = (roots_level, residual_level, image_level, second_level)
    for turn_of in range(1, members + len(stages) - 1):
        if turn_of == 1 and rounds > 0:
            relay_wait(rounds - 1)
        if turn_of < members:
            settle([1 + turn_of], True)
            assemble(1 + turn_of)
        together(*[stages[turn_of - m](m) for m in range(members) if 0 <= turn_of - m < len(stages)])

    lane_1 = iota((1, cols), 1)
    mine = jnp.zeros((1, cols), jnp.float32)
    for m in range(members):
        for q, acc in enumerate(grams[m]):
            mine = jnp.where(lane_1 == 4 * m + q, jnp.sum(acc, axis=1, keepdims=True), mine)
    gram_s[0] = mine


    def send_gram(d):
        px, py, pe = group_place(d)
        copy = pltpu.make_async_remote_copy(
            src_ref=gram_s, dst_ref=gram_r.at[pl.ds(d, 1)],
            send_sem=gram_send, recv_sem=gram_recv,
            device_id={"plane": px, "planey": py, "ens": pe}, device_id_type=mesh_id)
        own = (px == ix) & (py == iy) & (pe == ie)
        if isinstance(d, int) and d >= np_ * nq:
            copy.start()
        else:
            pl.when(jnp.logical_not(own))(copy.start)

    each_peer(send_gram)
    own_place = lax.rem(2 * ix + 1, np_) * nq + lax.rem(2 * iy + 1, nq)
    gram_r[pl.ds(own_place, 1)] = mine[None]

    def lie_down(src, dst):
        for c in range(2):
            flat_rows = jnp.concatenate(
                [src[c, q, pl.ds(TOP, cols)].T for q in range(2)], axis=0)
            for z in range(layers):
                dst[c, z] = flat_rows[SPAN * z:SPAN * z + rows]

    for m in range(members):
        lie_down(r_ext.at[m], r_core.at[m])
        send_r[m].start()
        lie_down(a_ext.at[m], a_core.at[m])
        send_a[m].start()
    everything = pltpu.make_async_remote_copy(
        src_ref=gram_blank, dst_ref=gram_blank, send_sem=gram_send, recv_sem=gram_recv,
        device_id=peer, device_id_type=mesh_id)
    everything.wait_recv()

    half = np_ * nq
    sums = [jnp.sum(gram_r[half * e:half * (e + 1)], axis=0) for e in range(ne)]
    steps = []
    for e in range(ne):
        for m in range(members):
            g_rr, g_ra, g_aa, g_ab = [
                jnp.sum(jnp.where(lane_1 == 4 * m + q, sums[e], 0.0), axis=1, keepdims=True)
                for q in range(4)
            ]
            first_step = g_rr / g_ra
            following = g_rr - 2.0 * first_step * g_ra + first_step * first_step * g_aa
            growth = 1.0 + following / g_rr
            curve = (growth * growth * g_ra - 2.0 * growth * first_step * g_aa
                     + first_step * first_step * g_ab)
            second_step = following / curve
            share = 1.0 / (members * ne)
            steps.append(((first_step + second_step * growth) * share,
                          second_step * first_step * share))

    peer_part = wide_blank.at[pl.ds(0, 1 + 2 * members)]
    peer_bulk = to_peer(peer_part, peer_part)
    peer_bulk.wait_recv()
    share = 1.0 / (members * ne)

    def final_step(z):
        for c in range(2):
            value = share * (w_core[c, z] + w_peer[c, z])
            for m in range(members):
                one, two = steps[m]
                value = value + one * r_core[m, c, z] - two * a_core[m, c, z]
                one, two = steps[members + m]
                value = value + one * r_peer[m, c, z] - two * a_peer[m, c, z]
            out_ref[c, z] = value

    for z in range(layers):
        final_step(z)

    settle(list(chunks), False)
    peer_bulk.wait_send()
    everything.wait_send()


def body(sizes, u_prior, friction_rows, friction_table, bed_fixed, ice_mask):
    members, _, layers, rows, cols = u_prior.shape
    levels = friction_table.shape[0]
    total = sizes[0] * sizes[1] * sizes[2]
    fixed = 2 + members
    pairs = (fixed + fixed % 2 + members * 2 * layers) // 2
    fields, lanes = 2 * members + 1, 2 * cols
    rounds = max(max(sizes[0], sizes[1]) - 2, 2)
    f32 = jnp.float32
    matrices = jnp.asarray(stencils(layers, lanes), jnp.bfloat16)
    any_space = pl.BlockSpec(memory_space=pl.ANY)
    vmem = lambda *shape: pltpu.VMEM(shape, f32)
    core = (members, 2, layers, rows, cols)
    tall = (2, PAD, cols)
    each = (members, 2) + tall
    inputs = (friction_rows, u_prior.reshape((-1,) + u_prior.shape[2:]), friction_table, bed_fixed, ice_mask, matrices)
    return pl.pallas_call(
        functools.partial(kernel, sizes),
        out_shape=pltpu.VMEM((2, layers, rows, cols), f32),
        in_specs=[any_space] * 6,
        out_specs=pl.BlockSpec(memory_space=pltpu.VMEM),
        scratch_shapes=[
            pltpu.SMEM((members,), jnp.int32), vmem(fields, layers + 1, SPAN, cols),
            vmem(levels, rows, cols),
            pltpu.VMEM((rows, cols), jnp.int32), pltpu.VMEM((rows, cols), jnp.int32),
            pltpu.VMEM(matrices.shape, jnp.bfloat16),
            vmem(pairs, 8, cols), vmem(pairs, 8, cols),
            vmem(2, members + 1, 2, 8, cols), vmem(2, 2, members + 1, 8, cols),
            vmem(pairs, 8, cols), vmem(pairs, 8, cols),
            vmem(2, members + 1, 2, 8, cols), vmem(2, 2, members + 1, 8, cols),
            vmem(members, layers + 1, SPAN, cols), vmem(fields, *tall), vmem(members, *tall),
            vmem(*tall), vmem(members, *tall),
            vmem(*each), vmem(*each), vmem(*each), vmem(*each), vmem(*each),
            vmem(2 + members, TALL, lanes),
            vmem(*core[1:]), vmem(*core), vmem(*core), vmem(*core), vmem(*core), vmem(*core[1:]),
            vmem(1, 1, cols), vmem(total, 1, cols), vmem(total - 1, 1, cols), vmem(2 * pairs + 8 * (members + 1), 8, cols),
            vmem(1 + 2 * members, *core[1:]),
            pltpu.SemaphoreType.REGULAR((rounds,)),
            pltpu.SemaphoreType.DMA((6,)),
            pltpu.SemaphoreType.DMA((members + 1,)), pltpu.SemaphoreType.DMA, pltpu.SemaphoreType.DMA,
        ],
        compiler_params=pltpu.CompilerParams(
            collective_id=0, has_side_effects=True, vmem_limit_bytes=40 << 20),
        name="picard",
    )(*[pltpu.with_memory_space_constraint(x, pltpu.HBM) for x in inputs])


def solution(mesh):
    sizes = (mesh.shape["plane"], mesh.shape["planey"], mesh.shape["ens"])
    in_specs = (
        P(("group", "ens"), None, None, "plane", "planey"),
        P(("group", "ens")),
        P("group", "plane", "planey"),
        P("plane", "planey"),
        P("plane", "planey"),
    )
    out_specs = P("group", None, "plane", "planey")
    return jax.shard_map(functools.partial(body, sizes), mesh=mesh, in_specs=in_specs,
                         out_specs=out_specs, check_vma=False)
```
